32 devices in a mesh: data: 32 (over z, y, x, core).
Axes of the slice: x: 2, y: 2, z: 4, core: 2. Of those that a mesh axis runs over, the one named last changes fastest.
Arguments:
- tokens: bfloat16 [65536, 768], P('data')
- upstream: bfloat16 [65536, 768], P('data')
- norm_gain: bfloat16 [2, 768], replicated
- w_up: bfloat16 [2, 768, 3072], replicated
- bias_up: bfloat16 [2, 3072], replicated
- w_down: bfloat16 [2, 3072, 768], replicated
- bias_down: bfloat16 [2, 768], replicated
Outputs:
- output 1: float32 [2, 768], replicated
- output 2: float32 [2, 768, 3072], replicated
- output 3: float32 [2, 3072], replicated
- output 4: float32 [2, 3072, 768], replicated
- output 5: float32 [2, 768], replicated
All inputs are finite; a program needn't handle non-finite values.
Results may differ from the reference program's by a relative error of at most 0.00727116.
Values are sent between devices in bfloat16 or wider.
A program may use at most 1 GiB of HBM per device.

```python
import jax
import jax.numpy as jnp
from jax import lax

D = 768
HIDDEN = 3072
LAYERS = 2
TOK_DEV = 2048
GROUP_SIZE = 32
TOKENS = GROUP_SIZE * TOK_DEV
EPSILON = 1e-6


def setup_inputs(seed: int = 0) -> dict:
    key_list = jax.random.split(jax.random.key(seed), 7)
    tokens = jax.random.normal(key_list[0], (TOKENS, D), jnp.float32)
    upstream = jax.random.normal(key_list[1], (TOKENS, D), jnp.float32) * (TOKENS ** -0.5)
    norm_gain = 1.0 + 0.5 * jax.random.normal(key_list[2], (LAYERS, D), jnp.float32)
    w_up = jax.random.normal(key_list[3], (LAYERS, D, HIDDEN), jnp.float32) * (D ** -0.5)
    bias_up = 0.5 * jax.random.normal(key_list[4], (LAYERS, HIDDEN), jnp.float32)
    w_down = jax.random.normal(key_list[5], (LAYERS, HIDDEN, D), jnp.float32) * (HIDDEN ** -0.5)
    bias_down = 0.5 * jax.random.normal(key_list[6], (LAYERS, D), jnp.float32)
    return {
        "tokens": tokens.astype(jnp.bfloat16),
        "upstream": upstream.astype(jnp.bfloat16),
        "norm_gain": norm_gain.astype(jnp.bfloat16),
        "w_up": w_up.astype(jnp.bfloat16),
        "bias_up": bias_up.astype(jnp.bfloat16),
        "w_down": w_down.astype(jnp.bfloat16),
        "bias_down": bias_down.astype(jnp.bfloat16),
    }


def gelu_tanh(values):
    return jax.nn.gelu(values, approximate=True)


def inverse_rms(hid_f):
    return lax.rsqrt(jnp.mean(hid_f * hid_f, axis=-1, keepdims=True) + EPSILON)


def shard_grads(tok_rows, up_rows, norm_gain, w_up, bias_up, w_down, bias_down):

    def forward_layer(hidden, layer_inputs):
        gain_row, up_mat, up_bias, down_mat, down_bias = layer_inputs
        hid_f = hidden.astype(jnp.float32)
        normed = (hid_f * inverse_rms(hid_f) * gain_row.astype(jnp.float32)).astype(jnp.bfloat16)
        pre_act = (jnp.dot(normed, up_mat, preferred_element_type=jnp.float32) + up_bias.astype(jnp.float32)).astype(jnp.bfloat16)
        activated = gelu_tanh(pre_act.astype(jnp.float32)).astype(jnp.bfloat16)
        branch = jnp.dot(activated, down_mat, preferred_element_type=jnp.float32)
        new_hidden = (hid_f + branch + down_bias.astype(jnp.float32)).astype(jnp.bfloat16)
        return new_hidden, (hidden, normed, pre_act, activated)

    top_hidden, saved_acts = lax.scan(forward_layer, tok_rows, (norm_gain, w_up, bias_up, w_down, bias_down))
    top_f = top_hidden.astype(jnp.float32)
    top_scale = inverse_rms(top_f)
    top_hat = top_f * top_scale
    up_f = up_rows.astype(jnp.float32)
    grad_top = top_scale * (up_f - top_hat * jnp.mean(up_f * top_hat, axis=-1, keepdims=True))

    def backward_layer(grad_h, layer_inputs):
        gain_row, up_mat, down_mat, hidden, normed, pre_act, activated = layer_inputs
        grad_b = grad_h.astype(jnp.bfloat16)
        grad_down = jnp.dot(activated.T, grad_b, preferred_element_type=jnp.float32)
        grad_down_bias = jnp.sum(grad_h, axis=0)
        grad_act = jnp.dot(grad_b, down_mat.T, preferred_element_type=jnp.float32)
        gelu_back = jax.vjp(gelu_tanh, pre_act.astype(jnp.float32))[1]
        grad_pre = gelu_back(grad_act)[0]
        grad_pre_b = grad_pre.astype(jnp.bfloat16)
        grad_up = jnp.dot(normed.T, grad_pre_b, preferred_element_type=jnp.float32)
        grad_up_bias = jnp.sum(grad_pre, axis=0)
        grad_normed = jnp.dot(grad_pre_b, up_mat.T, preferred_element_type=jnp.float32)
        hid_f = hidden.astype(jnp.float32)
        hid_scale = inverse_rms(hid_f)
        hid_hat = hid_f * hid_scale
        grad_gain = jnp.sum(grad_normed * hid_hat, axis=0)
        grad_hat = grad_normed * gain_row.astype(jnp.float32)
        grad_new = grad_h + hid_scale * (grad_hat - hid_hat * jnp.mean(grad_hat * hid_hat, axis=-1, keepdims=True))
        return grad_new, (grad_gain, grad_up, grad_up_bias, grad_down, grad_down_bias)

    saved_h, saved_n, saved_u, saved_a = saved_acts
    layer_grads = lax.scan(backward_layer, grad_top, (norm_gain, w_up, w_down, saved_h, saved_n, saved_u, saved_a), reverse=True)[1]
    return layer_grads


def reference(tokens, upstream, norm_gain, w_up, bias_up, w_down, bias_down):
    tok_shards = tokens.reshape(GROUP_SIZE, TOK_DEV, D)
    up_shards = upstream.reshape(GROUP_SIZE, TOK_DEV, D)
    zero_grads = (
        jnp.zeros((LAYERS, D), jnp.float32),
        jnp.zeros((LAYERS, D, HIDDEN), jnp.float32),
        jnp.zeros((LAYERS, HIDDEN), jnp.float32),
        jnp.zeros((LAYERS, HIDDEN, D), jnp.float32),
        jnp.zeros((LAYERS, D), jnp.float32),
    )

    def add_shard(running, shard_pair):
        shard_part = shard_grads(shard_pair[0], shard_pair[1], norm_gain, w_up, bias_up, w_down, bias_down)
        return tuple(run_sum + new_part for run_sum, new_part in zip(running, shard_part)), None

    running = lax.scan(add_shard, zero_grads, (tok_shards, up_shards))[0]
    return (running[0], running[1], running[2], running[3], running[4])
```

```python
import functools

import jax
import jax.numpy as jnp
from jax import lax
from jax.experimental import pallas as pl
from jax.experimental.pallas import tpu as pltpu
from jax.sharding import PartitionSpec as P

EPSILON = 1e-6
TOKEN_DIMS = (((0,), (0,)), ((), ()))
FEATURE_DIMS = (((1,), (1,)), ((), ()))
MESH = pl.DeviceIdType.MESH

SET_ROWS = 64
LAG = 2
SLOTS = 8
FIN_SLOTS = 16
STAGES = 11


def gelu_tanh(values):
    return jax.nn.gelu(values, approximate=True)


def inverse_rms(hid_f):
    return lax.rsqrt(jnp.mean(hid_f * hid_f, axis=-1, keepdims=True) + EPSILON)


def forward_stack(hidden, norm_gain, w_up, bias_up, w_down, bias_down):
    saved_acts = []
    for layer_idx in range(norm_gain.shape[0]):
        hid_f = hidden.astype(jnp.float32)
        hid_scale = inverse_rms(hid_f)
        hid_hat = hid_f * hid_scale
        normed = (hid_hat * norm_gain[layer_idx].astype(jnp.float32)).astype(jnp.bfloat16)
        pre_act = (jnp.dot(normed, w_up[layer_idx], preferred_element_type=jnp.float32) + bias_up[layer_idx].astype(jnp.float32)).astype(jnp.bfloat16)
        activated = gelu_tanh(pre_act.astype(jnp.float32)).astype(jnp.bfloat16)
        branch = jnp.dot(activated, w_down[layer_idx], preferred_element_type=jnp.float32)
        hidden = (hid_f + branch + bias_down[layer_idx].astype(jnp.float32)).astype(jnp.bfloat16)
        saved_acts.append((hid_scale, hid_hat, normed, pre_act, activated))
    return hidden, saved_acts


def top_gradient(top_hidden, upstream):
    top_f = top_hidden.astype(jnp.float32)
    top_scale = inverse_rms(top_f)
    top_hat = top_f * top_scale
    up_f = upstream.astype(jnp.float32)
    return top_scale * (up_f - top_hat * jnp.mean(up_f * top_hat, axis=-1, keepdims=True))


def layer_backward(grad_h, saved_layer, gain_row, up_mat, down_mat, need_input):
    hid_scale, hid_hat, normed, pre_act, activated = saved_layer
    grad_b = grad_h.astype(jnp.bfloat16)
    grad_down = lax.dot_general(activated, grad_b, TOKEN_DIMS, preferred_element_type=jnp.float32)
    grad_down_bias = jnp.sum(grad_h, axis=0)
    grad_act = lax.dot_general(grad_b, down_mat, FEATURE_DIMS, preferred_element_type=jnp.float32)
    gelu_back = jax.vjp(gelu_tanh, pre_act.astype(jnp.float32))[1]
    grad_pre = gelu_back(grad_act)[0]
    grad_pre_b = grad_pre.astype(jnp.bfloat16)
    grad_up = lax.dot_general(normed, grad_pre_b, TOKEN_DIMS, preferred_element_type=jnp.float32)
    grad_up_bias = jnp.sum(grad_pre, axis=0)
    grad_normed = lax.dot_general(grad_pre_b, up_mat, FEATURE_DIMS, preferred_element_type=jnp.float32)
    grad_gain = jnp.sum(grad_normed * hid_hat, axis=0)
    layer_grads = (grad_gain, grad_up, grad_up_bias, grad_down, grad_down_bias)
    if not need_input:
        return layer_grads, None
    grad_hat = grad_normed * gain_row.astype(jnp.float32)
    grad_new = grad_h + hid_scale * (grad_hat - hid_hat * jnp.mean(grad_hat * hid_hat, axis=-1, keepdims=True))
    return layer_grads, grad_new


def sum_kernel(axis, num_sets, per_mat, pd1, pu1, pd0, pu0, small, out_d, out_u, out_s,
               acc, fin, land0, land1, land2, land3, land4, land5, send_sem, recv_sem, loc_sem):
    width = acc.shape[2]
    half = SET_ROWS // 2
    piece = SET_ROWS // 8
    me = lax.axis_index(axis)
    core = lax.rem(me, 2)
    x = lax.rem(me // 2, 2)
    y = lax.rem(me // 4, 2)
    z = me // 8
    side = z // 2
    inner = jnp.logical_or(z == 1, z == 2)
    outer = jnp.logical_not(inner)
    b1 = jnp.where(core == 0, x, y)
    step1 = jnp.where(core == 0, 2, 4)
    b2 = jnp.where(core == 0, y, x)
    step2 = jnp.where(core == 0, 4, 2)
    partner = me + 1 - 2 * core
    near1 = me + step1 * (1 - 2 * b1)
    near2 = me + step2 * (1 - 2 * b2)
    zpair = me + 8 * (1 - 2 * lax.rem(z, 2))
    zmid = me + 8 * (3 - 2 * z)

    own_half = pl.multiple_of(b1 * half, 8)
    far_half = pl.multiple_of((1 - b1) * half, 8)
    start3 = pl.multiple_of(own_half + (1 - side) * piece, 8)
    far2 = pl.multiple_of(own_half + (1 - side) * 2 * piece, 8)
    near_2 = pl.multiple_of(own_half + side * 2 * piece, 8)
    outer_piece = pl.multiple_of(own_half + side * 3 * piece, 8)
    own_piece = pl.multiple_of(own_half + z * piece, 8)

    barrier = pltpu.get_barrier_semaphore()
    for peer in (partner, near1, near2, zpair):
        pl.semaphore_signal(barrier, inc=1, device_id=(peer,), device_id_type=MESH)

    @pl.when(inner)
    def _():
        pl.semaphore_signal(barrier, inc=1, device_id=(zmid,), device_id_type=MESH)

    pl.semaphore_wait(barrier, jnp.where(inner, 5, 4))

    def slot_of(k):
        return lax.rem(k, SLOTS)

    def copy_to(stage, k, src, dst, peer):
        slot = slot_of(k)
        return pltpu.make_async_remote_copy(
            src_ref=src, dst_ref=dst, send_sem=send_sem.at[stage, slot], recv_sem=recv_sem.at[stage, slot],
            device_id=(peer,), device_id_type=MESH)

    def rows_of(k, base, n):
        return acc.at[k, pl.ds(base, n), :]

    def done_of(k, base, n):
        return fin.at[lax.rem(k, FIN_SLOTS), pl.ds(base, n), :]

    def add_rows(k, base, n, land):
        acc[k, pl.ds(base, n), :] = acc[k, pl.ds(base, n), :] + land[slot_of(k)]

    def place(mat, j, who):
        if mat % 2 == 0:
            return pl.ds(pl.multiple_of(j * 2 * SET_ROWS + who * SET_ROWS, SET_ROWS), SET_ROWS), pl.ds(0, width)
        blocks = width // (2 * SET_ROWS)
        col = pl.multiple_of((j // blocks) * width, width)
        row = pl.multiple_of(lax.rem(j, blocks) * 2 * SET_ROWS + who * SET_ROWS, SET_ROWS)
        return pl.ds(row, SET_ROWS), pl.ds(col, width)

    def by_matrix(k, fn):
        for mat in range(4):
            @pl.when(jnp.logical_and(k >= mat * per_mat, k < (mat + 1) * per_mat))
            def _(mat=mat):
                fn(mat, k - mat * per_mat)

        @pl.when(k >= 4 * per_mat)
        def _():
            fn(4, None)

    def source(mat, j, who):
        if mat == 4:
            return small.at[pl.ds(pl.multiple_of(who * SET_ROWS, SET_ROWS), SET_ROWS), :]
        rows, cols = place(mat, j, who)
        return (pd1, pu1, pd0, pu0)[mat].at[rows, cols]

    def target(mat, j, who):
        if mat == 4:
            return out_s.at[pl.ds(pl.multiple_of(who * SET_ROWS, SET_ROWS), SET_ROWS), :]
        rows, cols = place(mat, j, who)
        return (out_d if mat % 2 == 0 else out_u).at[1 - mat // 2, rows, cols]

    def c_pair(k, mat=4, j=None):
        return copy_to(0, k, source(mat, j, 1 - core), land0.at[slot_of(k)], partner)

    def c_mine(k, mat=4, j=None):
        return pltpu.make_async_copy(source(mat, j, core), acc.at[k], loc_sem.at[0, slot_of(k)])

    def c_d1(k):
        return copy_to(1, k, rows_of(k, far_half, half), land1.at[slot_of(k)], near1)

    def c_za(k):
        return copy_to(2, k, rows_of(k, start3, 3 * piece), land2.at[slot_of(k)], zpair)

    def c_zb(k):
        return copy_to(3, k, rows_of(k, far2, 2 * piece), land3.at[slot_of(k)], zmid)

    def c_zc(k):
        return copy_to(4, k, rows_of(k, outer_piece, piece), land4.at[slot_of(k)], zpair)

    def c_d2(k):
        return copy_to(5, k, rows_of(k, own_piece, piece), land5.at[slot_of(k)], near2)

    def c_zd(k):
        return copy_to(6, k, done_of(k, outer_piece, piece), done_of(k, outer_piece, piece), zpair)

    def c_ze(k):
        return copy_to(7, k, done_of(k, near_2, 2 * piece), done_of(k, near_2, 2 * piece), zmid)

    def c_zf(k):
        return copy_to(8, k, done_of(k, start3, 3 * piece), done_of(k, start3, 3 * piece), zpair)

    def c_e1(k):
        return copy_to(9, k, done_of(k, own_half, half), done_of(k, own_half, half), near1)

    def c_out(k, mat=4, j=None):
        return copy_to(10, k, done_of(k, 0, SET_ROWS), target(mat, j, core), partner)

    def c_loc(k, mat=4, j=None):
        return pltpu.make_async_copy(done_of(k, 0, SET_ROWS), target(mat, j, core), loc_sem.at[1, slot_of(k)])

    def wait0(k):
        pass

    def send0(k):
        def go(mat, j):
            c_pair(k, mat, j).start()
            c_mine(k, mat, j).start()
        by_matrix(k, go)

    def wait1(k):
        c_pair(k).wait()
        c_mine(k).wait()
        add_rows(k, 0, SET_ROWS, land0)

    def send1(k):
        c_d1(k).start()

    def wait2(k):
        c_d1(k).wait()
        add_rows(k, own_half, half, land1)

    def send2(k):
        @pl.when(outer)
        def _():
            c_za(k).start()

    def wait3(k):
        @pl.when(inner)
        def _():
            c_za(k).wait_recv()
            add_rows(k, start3, 3 * piece, land2)

        @pl.when(outer)
        def _():
            c_za(k).wait_send()

    def send3(k):
        @pl.when(inner)
        def _():
            c_zb(k).start()

    def wait4(k):
        @pl.when(inner)
        def _():
            c_zb(k).wait()
            add_rows(k, near_2, 2 * piece, land3)

    def send4(k):
        @pl.when(inner)
        def _():
            c_zc(k).start()

    def wait5(k):
        @pl.when(inner)
        def _():
            c_zc(k).wait_send()

        @pl.when(outer)
        def _():
            c_zc(k).wait_recv()
            add_rows(k, outer_piece, piece, land4)

    def send5(k):
        c_d2(k).start()

    def wait6(k):
        c_d2(k).wait()
        fin[lax.rem(k, FIN_SLOTS), pl.ds(own_piece, piece), :] = acc[k, pl.ds(own_piece, piece), :] + land5[slot_of(k)]

    def send6(k):
        @pl.when(outer)
        def _():
            c_zd(k).start()

    def wait7(k):
        @pl.when(inner)
        def _():
            c_zd(k).wait_recv()

        @pl.when(outer)
        def _():
            c_zd(k).wait_send()

    def send7(k):
        @pl.when(inner)
        def _():
            c_ze(k).start()

    def wait8(k):
        @pl.when(inner)
        def _():
            c_ze(k).wait()

    def send8(k):
        @pl.when(inner)
        def _():
            c_zf(k).start()

    def wait9(k):
        @pl.when(inner)
        def _():
            c_zf(k).wait_send()

        @pl.when(outer)
        def _():
            c_zf(k).wait_recv()

    def send9(k):
        c_e1(k).start()

    def wait10(k):
        c_e1(k).wait()

    def send10(k):
        def go(mat, j):
            c_out(k, mat, j).start()
            c_loc(k, mat, j).start()
        by_matrix(k, go)

    def wait11(k):
        c_out(k).wait()
        c_loc(k).wait()

    def send11(k):
        pass

    waits = [wait0, wait1, wait2, wait3, wait4, wait5, wait6, wait7, wait8, wait9, wait10, wait11]
    sends = [send0, send1, send2, send3, send4, send5, send6, send7, send8, send9, send10, send11]

    def tick(t):
        for stage in range(STAGES, -1, -1):
            k = t - stage * LAG

            @pl.when(jnp.logical_and(k >= 0, k < num_sets))
            def _(k=k, stage=stage):
                waits[stage](k)
                sends[stage](k)

    pl.loop(0, num_sets + STAGES * LAG)(tick)


def sum_over_devices(axis, pd1, pu1, pd0, pu0, small):
    hidden, width = pd1.shape
    per_mat = hidden // (2 * SET_ROWS)
    num_sets = 4 * per_mat + 1
    piece = SET_ROWS // 8
    any_spec = pl.BlockSpec(memory_space=pl.ANY)
    f32 = jnp.float32
    return pl.pallas_call(
        functools.partial(sum_kernel, axis, num_sets, per_mat),
        name="sum_over_devices",
        out_shape=[jax.ShapeDtypeStruct((2, hidden, width), f32), jax.ShapeDtypeStruct((2, width, hidden), f32),
                   jax.ShapeDtypeStruct(small.shape, f32)],
        in_specs=[any_spec] * 5,
        out_specs=[any_spec] * 3,
        scratch_shapes=[
            pltpu.VMEM((num_sets, SET_ROWS, width), f32),
            pltpu.VMEM((FIN_SLOTS, SET_ROWS, width), f32),
            pltpu.VMEM((SLOTS, SET_ROWS, width), f32),
            pltpu.VMEM((SLOTS, SET_ROWS // 2, width), f32),
            pltpu.VMEM((SLOTS, 3 * piece, width), f32),
            pltpu.VMEM((SLOTS, 2 * piece, width), f32),
            pltpu.VMEM((SLOTS, piece, width), f32),
            pltpu.VMEM((SLOTS, piece, width), f32),
            pltpu.SemaphoreType.DMA((STAGES, SLOTS)),
            pltpu.SemaphoreType.DMA((STAGES, SLOTS)),
            pltpu.SemaphoreType.DMA((2, SLOTS)),
        ],
        compiler_params=pltpu.CompilerParams(collective_id=0, has_side_effects=True, vmem_limit_bytes=40 * 1024 * 1024),
    )(pd1, pu1, pd0, pu0, small)


def solution(mesh):
    data_axis = mesh.axis_names[0]

    def device_grads(tokens, upstream, norm_gain, w_up, bias_up, w_down, bias_down):
        top_hidden, saved_acts = forward_stack(tokens, norm_gain, w_up, bias_up, w_down, bias_down)
        grad_h = top_gradient(top_hidden, upstream)
        num_layers = norm_gain.shape[0]
        grads = [None] * num_layers
        for layer_idx in reversed(range(num_layers)):
            grads[layer_idx], grad_h = layer_backward(grad_h, saved_acts[layer_idx], norm_gain[layer_idx], w_up[layer_idx], w_down[layer_idx], layer_idx > 0)
        width = norm_gain.shape[1]
        blocks = bias_up.shape[1] // width
        rows = []
        for layer_idx in range(num_layers):
            gain, _, up_bias, _, down_bias = grads[layer_idx]
            rows += [gain[None], up_bias.reshape(blocks, width), down_bias[None]]
        small = jnp.concatenate(rows, axis=0)
        small = jnp.pad(small, ((0, 2 * SET_ROWS - small.shape[0]), (0, 0)))
        out_d, out_u, out_s = sum_over_devices(data_axis, grads[1][3], grads[1][1], grads[0][3], grads[0][1], small)
        per = blocks + 2
        layers = out_s[: num_layers * per].reshape(num_layers, per, width)
        return (layers[:, 0], out_u, layers[:, 1 : 1 + blocks].reshape(num_layers, blocks * width), out_d, layers[:, 1 + blocks])

    row_spec = P(data_axis, None)
    full_spec = P()
    return jax.shard_map(
        device_grads,
        mesh=mesh,
        in_specs=(row_spec, row_spec, full_spec, full_spec, full_spec, full_spec, full_spec),
        out_specs=(full_spec, full_spec, full_spec, full_spec, full_spec),
        check_vma=False,
    )
```

```python
import functools

import jax
import jax.numpy as jnp
from jax import lax
from jax.experimental import pallas as pl
from jax.experimental.pallas import tpu as pltpu
from jax.sharding import PartitionSpec as P

EPSILON = 1e-6
GELU_C = 0.7978845608028654
GELU_A = 0.044715
MESH = pl.DeviceIdType.MESH
bf16 = jnp.bfloat16
f32 = jnp.float32

ROW_TILE = 512
CHUNK = 512
SET_ROWS = 64
LAG = 2
SLOTS = 8
FIN_SLOTS = 16
STAGES = 11


def gelu_f32(u):
    inner = u * (GELU_C + (GELU_C * GELU_A) * (u * u))
    half = 0.5 * u
    return half + half * jnp.tanh(inner)


def forward_kernel(tok, up, gain, wu, bu, wd, bd, u_out, a_out, h_out, n_out, g_out, gb_out, hid):
    layer = pl.program_id(0)
    r = pl.program_id(1)
    rows = pl.ds(pl.multiple_of(r * ROW_TILE, ROW_TILE), ROW_TILE)

    @pl.when(layer == 0)
    def _():
        hid[rows, :] = tok[...]

    xb = hid[rows, :]
    x = xb.astype(f32)
    scale = lax.rsqrt(jnp.mean(x * x, axis=-1, keepdims=True) + EPSILON)
    n = ((x * scale) * gain[0].astype(f32)).astype(bf16)
    h_out[0] = xb
    n_out[0] = n
    hidden = wu.shape[2]
    acc = None
    for j in range(hidden // CHUNK):
        cols = pl.ds(j * CHUNK, CHUNK)
        pre = jnp.dot(n, wu[0, :, cols], preferred_element_type=f32) + bu[0, :, cols].astype(f32)
        u = pre.astype(bf16)
        u_out[0, :, cols] = u
        a = gelu_f32(u.astype(f32)).astype(bf16)
        a_out[0, :, cols] = a
        part = jnp.dot(a, wd[0, cols, :], preferred_element_type=f32)
        acc = part if acc is None else acc + part
    new = ((x + acc) + bd[0].astype(f32)).astype(bf16)
    hid[rows, :] = new

    @pl.when(layer == 1)
    def _():
        top = new.astype(f32)
        s = lax.rsqrt(jnp.mean(top * top, axis=-1, keepdims=True) + EPSILON)
        zt = top * s
        upf = up[...].astype(f32)
        g = s * (upf - zt * jnp.mean(upf * zt, axis=-1, keepdims=True))
        g_out[...] = g
        gb_out[...] = g.astype(bf16)


def forward(tokens, upstream, norm_gain, w_up, bias_up, w_down, bias_down):
    rows, width = tokens.shape
    layers, _, hidden = w_up.shape
    tm = ROW_TILE
    grid = (layers, rows // tm)
    return pl.pallas_call(
        forward_kernel,
        name="forward",
        grid=grid,
        in_specs=[
            pl.BlockSpec((tm, width), lambda l, r: (r * (1 - l), 0)),
            pl.BlockSpec((tm, width), lambda l, r: (r * l, 0)),
            pl.BlockSpec((1, 1, width), lambda l, r: (l, 0, 0)),
            pl.BlockSpec((1, width, hidden), lambda l, r: (l, 0, 0)),
            pl.BlockSpec((1, 1, hidden), lambda l, r: (l, 0, 0)),
            pl.BlockSpec((1, hidden, width), lambda l, r: (l, 0, 0)),
            pl.BlockSpec((1, 1, width), lambda l, r: (l, 0, 0)),
        ],
        out_specs=[
            pl.BlockSpec((1, tm, hidden), lambda l, r: (l, r, 0)),
            pl.BlockSpec((1, tm, hidden), lambda l, r: (l, r, 0)),
            pl.BlockSpec((1, tm, width), lambda l, r: (l, r, 0)),
            pl.BlockSpec((1, tm, width), lambda l, r: (l, r, 0)),
            pl.BlockSpec((tm, width), lambda l, r: (r * l, 0)),
            pl.BlockSpec((tm, width), lambda l, r: (r * l, 0)),
        ],
        out_shape=[
            jax.ShapeDtypeStruct((layers, rows, hidden), bf16),
            jax.ShapeDtypeStruct((layers, rows, hidden), bf16),
            jax.ShapeDtypeStruct((layers, rows, width), bf16),
            jax.ShapeDtypeStruct((layers, rows, width), bf16),
            jax.ShapeDtypeStruct((rows, width), f32),
            jax.ShapeDtypeStruct((rows, width), bf16),
        ],
        scratch_shapes=[pltpu.VMEM((rows, width), bf16)],
        compiler_params=pltpu.CompilerParams(vmem_limit_bytes=60 * 1024 * 1024, dimension_semantics=("arbitrary", "arbitrary")),
    )(tokens, upstream, norm_gain[:, None, :], w_up, bias_up[:, None, :], w_down, bias_down[:, None, :])


def backward_kernel(axis, num_sets, per_mat, g_hbm, gb_hbm, a_hbm, u_hbm, n_hbm, h_hbm, wd_hbm, wu_hbm, gain,
                    out_d, out_u, out_s, part_d, part_u, part_s,
                    acc, fin, land0, land1, land2, land3, land4, land5,
                    g, gb, m, xbuf, nbuf, hbuf, wd, wu, dbuf, rbuf, sbuf,
                    send_sem, recv_sem, loc_sem, x_sem, w_sem, r_sem, in_sem):
    width = acc.shape[2]
    half = SET_ROWS // 2
    piece = SET_ROWS // 8
    me = lax.axis_index(axis)
    core = lax.rem(me, 2)
    x = lax.rem(me // 2, 2)
    y = lax.rem(me // 4, 2)
    z = me // 8
    side = z // 2
    inner = jnp.logical_or(z == 1, z == 2)
    outer = jnp.logical_not(inner)
    b1 = jnp.where(core == 0, x, y)
    step1 = jnp.where(core == 0, 2, 4)
    b2 = jnp.where(core == 0, y, x)
    step2 = jnp.where(core == 0, 4, 2)
    partner = me + 1 - 2 * core
    near1 = me + step1 * (1 - 2 * b1)
    near2 = me + step2 * (1 - 2 * b2)
    zpair = me + 8 * (1 - 2 * lax.rem(z, 2))
    zmid = me + 8 * (3 - 2 * z)

    own_half = pl.multiple_of(b1 * half, 8)
    far_half = pl.multiple_of((1 - b1) * half, 8)
    start3 = pl.multiple_of(own_half + (1 - side) * piece, 8)
    far2 = pl.multiple_of(own_half + (1 - side) * 2 * piece, 8)
    near_2 = pl.multiple_of(own_half + side * 2 * piece, 8)
    outer_piece = pl.multiple_of(own_half + side * 3 * piece, 8)
    own_piece = pl.multiple_of(own_half + z * piece, 8)

    barrier = pltpu.get_barrier_semaphore()
    for peer in (partner, near1, near2, zpair):
        pl.semaphore_signal(barrier, inc=1, device_id=(peer,), device_id_type=MESH)

    @pl.when(inner)
    def _():
        pl.semaphore_signal(barrier, inc=1, device_id=(zmid,), device_id_type=MESH)

    pl.semaphore_wait(barrier, jnp.where(inner, 5, 4))

    def slot_of(k):
        return lax.rem(k, SLOTS)

    def copy_to(stage, k, src, dst, peer):
        slot = slot_of(k)
        return pltpu.make_async_remote_copy(
            src_ref=src, dst_ref=dst, send_sem=send_sem.at[stage, slot], recv_sem=recv_sem.at[stage, slot],
            device_id=(peer,), device_id_type=MESH)

    def rows_of(k, base, n):
        return acc.at[lax.rem(k, FIN_SLOTS), pl.ds(base, n), :]

    def done_of(k, base, n):
        return fin.at[lax.rem(k, FIN_SLOTS), pl.ds(base, n), :]

    def add_rows(k, base, n, land):
        slot = lax.rem(k, FIN_SLOTS)
        acc[slot, pl.ds(base, n), :] = acc[slot, pl.ds(base, n), :] + land[slot_of(k)]

    def place(kind, j, who):
        if kind == 0:
            return pl.ds(pl.multiple_of(j * 2 * SET_ROWS + who * SET_ROWS, SET_ROWS), SET_ROWS), pl.ds(0, width)
        blocks = width // (2 * SET_ROWS)
        col = pl.multiple_of((j // blocks) * width, width)
        row = pl.multiple_of(lax.rem(j, blocks) * 2 * SET_ROWS + who * SET_ROWS, SET_ROWS)
        return pl.ds(row, SET_ROWS), pl.ds(col, width)

    def by_matrix(k, fn):
        mat = k // per_mat
        j = lax.rem(k, per_mat)
        for kind in range(2):
            @pl.when(jnp.logical_and(mat < 4, lax.rem(mat, 2) == kind))
            def _(kind=kind):
                fn(kind, (1 - mat // 2, j))

        @pl.when(mat >= 4)
        def _():
            fn(2, None)

    def part_of(refs, kind, where, who):
        if kind == 2:
            return refs[2].at[pl.ds(pl.multiple_of(who * SET_ROWS, SET_ROWS), SET_ROWS), :]
        rows, cols = place(kind, where[1], who)
        return refs[kind].at[where[0], rows, cols]

    def source(kind, where, who):
        return part_of((part_d, part_u, part_s), kind, where, who)

    def target(kind, where, who):
        return part_of((out_d, out_u, out_s), kind, where, who)

    def c_pair(k, kind=2, where=None):
        return copy_to(0, k, source(kind, where, 1 - core), land0.at[slot_of(k)], partner)

    def c_mine(k, kind=2, where=None):
        return pltpu.make_async_copy(source(kind, where, core), acc.at[lax.rem(k, FIN_SLOTS)], loc_sem.at[0, slot_of(k)])

    def c_d1(k):
        return copy_to(1, k, rows_of(k, far_half, half), land1.at[slot_of(k)], near1)

    def c_za(k):
        return copy_to(2, k, rows_of(k, start3, 3 * piece), land2.at[slot_of(k)], zpair)

    def c_zb(k):
        return copy_to(3, k, rows_of(k, far2, 2 * piece), land3.at[slot_of(k)], zmid)

    def c_zc(k):
        return copy_to(4, k, rows_of(k, outer_piece, piece), land4.at[slot_of(k)], zpair)

    def c_d2(k):
        return copy_to(5, k, rows_of(k, own_piece, piece), land5.at[slot_of(k)], near2)

    def c_zd(k):
        return copy_to(6, k, done_of(k, outer_piece, piece), done_of(k, outer_piece, piece), zpair)

    def c_ze(k):
        return copy_to(7, k, done_of(k, near_2, 2 * piece), done_of(k, near_2, 2 * piece), zmid)

    def c_zf(k):
        return copy_to(8, k, done_of(k, start3, 3 * piece), done_of(k, start3, 3 * piece), zpair)

    def c_e1(k):
        return copy_to(9, k, done_of(k, own_half, half), done_of(k, own_half, half), near1)

    def c_out(k, kind=2, where=None):
        return copy_to(10, k, done_of(k, 0, SET_ROWS), target(kind, where, core), partner)

    def c_loc(k, kind=2, where=None):
        return pltpu.make_async_copy(done_of(k, 0, SET_ROWS), target(kind, where, core), loc_sem.at[1, slot_of(k)])

    def wait0(k):
        pass

    def send0(k):
        def go(kind, where):
            c_pair(k, kind, where).start()
            c_mine(k, kind, where).start()
        by_matrix(k, go)

    def wait1(k):
        c_pair(k).wait()
        c_mine(k).wait()
        add_rows(k, 0, SET_ROWS, land0)

    def send1(k):
        c_d1(k).start()

    def wait2(k):
        c_d1(k).wait()
        add_rows(k, own_half, half, land1)

    def send2(k):
        @pl.when(outer)
        def _():
            c_za(k).start()

    def wait3(k):
        @pl.when(inner)
        def _():
            c_za(k).wait_recv()
            add_rows(k, start3, 3 * piece, land2)

        @pl.when(outer)
        def _():
            c_za(k).wait_send()

    def send3(k):
        @pl.when(inner)
        def _():
            c_zb(k).start()

    def wait4(k):
        @pl.when(inner)
        def _():
            c_zb(k).wait()
            add_rows(k, near_2, 2 * piece, land3)

    def send4(k):
        @pl.when(inner)
        def _():
            c_zc(k).start()

    def wait5(k):
        @pl.when(inner)
        def _():
            c_zc(k).wait_send()

        @pl.when(outer)
        def _():
            c_zc(k).wait_recv()
            add_rows(k, outer_piece, piece, land4)

    def send5(k):
        c_d2(k).start()

    def wait6(k):
        c_d2(k).wait()
        slot = lax.rem(k, FIN_SLOTS)
        fin[slot, pl.ds(own_piece, piece), :] = acc[slot, pl.ds(own_piece, piece), :] + land5[slot_of(k)]

    def send6(k):
        @pl.when(outer)
        def _():
            c_zd(k).start()

    def wait7(k):
        @pl.when(inner)
        def _():
            c_zd(k).wait_recv()

        @pl.when(outer)
        def _():
            c_zd(k).wait_send()

    def send7(k):
        @pl.when(inner)
        def _():
            c_ze(k).start()

    def wait8(k):
        @pl.when(inner)
        def _():
            c_ze(k).wait()

    def send8(k):
        @pl.when(inner)
        def _():
            c_zf(k).start()

    def wait9(k):
        @pl.when(inner)
        def _():
            c_zf(k).wait_send()

        @pl.when(outer)
        def _():
            c_zf(k).wait_recv()

    def send9(k):
        c_e1(k).start()

    def wait10(k):
        c_e1(k).wait()

    def send10(k):
        def go(kind, where):
            c_out(k, kind, where).start()
            c_loc(k, kind, where).start()
        by_matrix(k, go)

    def wait11(k):
        c_out(k).wait()
        c_loc(k).wait()

    def send11(k):
        pass

    waits = [wait0, wait1, wait2, wait3, wait4, wait5, wait6, wait7, wait8, wait9, wait10, wait11]
    sends = [send0, send1, send2, send3, send4, send5, send6, send7, send8, send9, send10, send11]

    def tick(t):
        for stage in range(STAGES, -1, -1):
            k = t - stage * LAG

            @pl.when(jnp.logical_and(k >= 0, k < num_sets))
            def _(k=k, stage=stage):
                waits[stage](k)
                sends[stage](k)


    rows = g.shape[0]
    blocks = per_mat * 2 * SET_ROWS // width
    half_w = width // 2
    a_steps = 2 * blocks
    b_steps = 6 * blocks
    c_steps = 4
    layer_steps = a_steps + b_steps + c_steps
    all_steps = 2 * layer_steps
    tile = rows // 4
    small_rows = blocks + 2

    def load_x(q):
        layer = 1 - q // (2 * blocks)
        cols = pl.ds(pl.multiple_of(lax.rem(q, blocks) * width, width), width)
        for kind, ref in enumerate((a_hbm, u_hbm)):
            @pl.when(jnp.logical_and(q < 4 * blocks, lax.rem(q // blocks, 2) == kind))
            def _(ref=ref):
                pltpu.make_async_copy(ref.at[layer, :, cols], xbuf.at[lax.rem(q, 2)], x_sem.at[lax.rem(q, 2)]).start()

    def wait_x(q):
        pltpu.make_async_copy(a_hbm.at[0, :, pl.ds(0, width)], xbuf.at[lax.rem(q, 2)], x_sem.at[lax.rem(q, 2)]).wait()

    def w_copies(p):
        slot = lax.rem(p, 2)
        layer = 1 - p // blocks
        span = pl.ds(pl.multiple_of(lax.rem(p, blocks) * width, width), width)
        return (pltpu.make_async_copy(wd_hbm.at[layer, span, :], wd.at[slot], w_sem.at[0, slot]),
                pltpu.make_async_copy(wu_hbm.at[layer, :, span], wu.at[slot], w_sem.at[1, slot]))

    def layer_copies(layer):
        return (pltpu.make_async_copy(n_hbm.at[layer], nbuf, in_sem.at[2]), pltpu.make_async_copy(h_hbm.at[layer], hbuf, in_sem.at[3]))

    def result_wait(slot):
        pltpu.make_async_copy(rbuf.at[slot], part_d.at[0, pl.ds(0, half_w), :], r_sem.at[slot]).wait()

    load_gb = pltpu.make_async_copy(gb_hbm, gb, in_sem.at[0])
    load_g = pltpu.make_async_copy(g_hbm, g, in_sem.at[1])
    load_gb.start()
    load_x(jnp.int32(0))
    load_x(jnp.int32(1))
    for copy in w_copies(jnp.int32(0)):
        copy.start()
    load_g.start()
    sbuf[...] = jnp.zeros_like(sbuf)
    load_gb.wait()

    def step_a(layer, w, r):
        slot = lax.rem(w, 2)
        block = w // 2
        q = (1 - layer) * 2 * blocks + block

        @pl.when(w == 0)
        def _():
            for copy in layer_copies(layer):
                copy.start()
            m[...] = jnp.zeros_like(m)

        @pl.when(slot == 0)
        def _():
            wait_x(q)

        @pl.when(r >= 2)
        def _():
            result_wait(slot)

        cols = pl.ds(pl.multiple_of(slot * half_w, 128), half_w)
        rbuf[slot] = lax.dot_general(xbuf[lax.rem(q, 2), :, cols], gb[...], (((0,), (0,)), ((), ())), preferred_element_type=f32)
        out_rows = pl.ds(pl.multiple_of(w * half_w, 128), half_w)
        pltpu.make_async_copy(rbuf.at[slot], part_d.at[layer, out_rows, :], r_sem.at[slot]).start()

        @pl.when(slot == 1)
        def _():
            load_x(q + 2)

    def step_e(layer, block, i):
        q = (1 - layer) * 2 * blocks + blocks + block
        p = (1 - layer) * blocks + block

        @pl.when(i == 0)
        def _():
            wait_x(q)
            for copy in w_copies(p):
                copy.wait()

            @pl.when(p + 1 < 2 * blocks)
            def _():
                for copy in w_copies(p + 1):
                    copy.start()

        total = None
        for sub in range(2):
            span = pl.ds(pl.multiple_of((2 * i + sub) * tile, 16), tile)
            e = lax.dot_general(gb[span, :], wd[lax.rem(p, 2)], (((1,), (1,)), ((), ())), preferred_element_type=f32)
            u = xbuf[lax.rem(q, 2), span, :].astype(f32)
            sq = u * u
            t = jnp.tanh(u * (GELU_C + (GELU_C * GELU_A) * sq))
            slope = ((1.0 - t * t) * (0.5 * u)) * (GELU_C + (3.0 * GELU_C * GELU_A) * sq) + (0.5 + 0.5 * t)
            d = e * slope
            dbuf[span, :] = d.astype(bf16)
            col = jnp.sum(d, axis=0, keepdims=True)
            total = col if total is None else total + col
        row = pl.ds(layer * small_rows + 1 + block, 1)
        sbuf[row, :] = sbuf[row, :] + total

        @pl.when(i == 1)
        def _():
            load_x(q + 2)

    def step_m(layer, block, i):
        p = (1 - layer) * blocks + block
        span = pl.ds(pl.multiple_of(i * 2 * tile, 16), 2 * tile)
        m[span, :] = m[span, :] + lax.dot_general(dbuf[span, :], wu[lax.rem(p, 2)], (((1,), (1,)), ((), ())), preferred_element_type=f32)

    def step_u(layer, block, i):
        @pl.when(jnp.logical_and(block == 0, i == 0))
        def _():
            for copy in layer_copies(layer):
                copy.wait()

        result_wait(i)
        cols = pl.ds(pl.multiple_of(i * half_w, 128), half_w)
        rbuf[i] = lax.dot_general(nbuf[:, cols], dbuf[...], (((0,), (0,)), ((), ())), preferred_element_type=f32)
        out_cols = pl.ds(pl.multiple_of(block * width, width), width)
        pltpu.make_async_copy(rbuf.at[i], part_u.at[layer, cols, out_cols], r_sem.at[i]).start()

    def step_c(layer, i):
        @pl.when(jnp.logical_and(layer == 1, i == 0))
        def _():
            load_g.wait()

        span = pl.ds(pl.multiple_of(i * tile, 16), tile)
        x = hbuf[span, :].astype(f32)
        scale = lax.rsqrt(jnp.mean(x * x, axis=-1, keepdims=True) + EPSILON)
        hat = x * scale
        grad_n = m[span, :]
        old = g[span, :]
        gain_row = pl.ds(layer * small_rows, 1)
        bias_row = pl.ds(layer * small_rows + blocks + 1, 1)
        sbuf[gain_row, :] = sbuf[gain_row, :] + jnp.sum(grad_n * hat, axis=0, keepdims=True)
        sbuf[bias_row, :] = sbuf[bias_row, :] + jnp.sum(old, axis=0, keepdims=True)
        grad_hat = grad_n * gain[layer].astype(f32)
        new = old + scale * (grad_hat - hat * jnp.mean(grad_hat * hat, axis=-1, keepdims=True))
        g[span, :] = new
        gb[span, :] = new.astype(bf16)

    def compute(s):
        layer = 1 - s // layer_steps
        w = lax.rem(s, layer_steps)
        v = w - a_steps
        block = v // 6
        i = lax.rem(v, 2)
        what = lax.rem(v, 6) // 2
        r = (1 - layer) * 4 * blocks + w

        @pl.when(w < a_steps)
        def _():
            step_a(layer, w, r)

        in_b = jnp.logical_and(v >= 0, v < b_steps)
        for number, step in enumerate((step_e, step_m, step_u)):
            @pl.when(jnp.logical_and(in_b, what == number))
            def _(step=step):
                step(layer, block, i)

        @pl.when(v >= b_steps)
        def _():
            step_c(layer, v - b_steps)

    small_copy = pltpu.make_async_copy(sbuf, part_s, in_sem.at[4])

    def whole_step(s):
        @pl.when(s < all_steps)
        def _():
            compute(s)

        @pl.when(s == all_steps)
        def _():
            small_copy.start()
            result_wait(0)
            result_wait(1)
            small_copy.wait()

        @pl.when(s >= 2)
        def _():
            tick(s - 2)

    pl.loop(0, num_sets + STAGES * LAG + 2)(whole_step)


def backward(axis, g, gb, a, u, n, h, w_down, w_up, norm_gain):
    rows, width = g.shape
    hidden = a.shape[2]
    per_mat = hidden // (2 * SET_ROWS)
    num_sets = 4 * per_mat + 1
    piece = SET_ROWS // 8
    any_spec = pl.BlockSpec(memory_space=pl.ANY)
    shape = jax.ShapeDtypeStruct
    shapes = [shape((2, hidden, width), f32), shape((2, width, hidden), f32), shape((2 * SET_ROWS, width), f32)]
    return pl.pallas_call(
        functools.partial(backward_kernel, axis, num_sets, per_mat),
        name="backward_and_sum",
        out_shape=shapes + shapes,
        in_specs=[any_spec] * 8 + [pl.BlockSpec(memory_space=pltpu.VMEM)],
        out_specs=[any_spec] * 6,
        scratch_shapes=[
            pltpu.VMEM((FIN_SLOTS, SET_ROWS, width), f32),
            pltpu.VMEM((FIN_SLOTS, SET_ROWS, width), f32),
            pltpu.VMEM((SLOTS, SET_ROWS, width), f32),
            pltpu.VMEM((SLOTS, SET_ROWS // 2, width), f32),
            pltpu.VMEM((SLOTS, 3 * piece, width), f32),
            pltpu.VMEM((SLOTS, 2 * piece, width), f32),
            pltpu.VMEM((SLOTS, piece, width), f32),
            pltpu.VMEM((SLOTS, piece, width), f32),
            pltpu.VMEM((rows, width), f32),
            pltpu.VMEM((rows, width), bf16),
            pltpu.VMEM((rows, width), f32),
            pltpu.VMEM((2, rows, width), bf16),
            pltpu.VMEM((rows, width), bf16),
            pltpu.VMEM((rows, width), bf16),
            pltpu.VMEM((2, width, width), bf16),
            pltpu.VMEM((2, width, width), bf16),
            pltpu.VMEM((rows, width), bf16),
            pltpu.VMEM((2, width // 2, width), f32),
            pltpu.VMEM((2 * SET_ROWS, width), f32),
            pltpu.SemaphoreType.DMA((STAGES, SLOTS)),
            pltpu.SemaphoreType.DMA((STAGES, SLOTS)),
            pltpu.SemaphoreType.DMA((2, SLOTS)),
            pltpu.SemaphoreType.DMA((2,)),
            pltpu.SemaphoreType.DMA((2, 2)),
            pltpu.SemaphoreType.DMA((2,)),
            pltpu.SemaphoreType.DMA((5,)),
        ],
        compiler_params=pltpu.CompilerParams(collective_id=0, has_side_effects=True, vmem_limit_bytes=62 * 1024 * 1024),
    )(g, gb, a, u, n, h, w_down, w_up, norm_gain[:, None, :])


def solution(mesh):
    data_axis = mesh.axis_names[0]

    def device_grads(tokens, upstream, norm_gain, w_up, bias_up, w_down, bias_down):
        u, a, h, n, g, gb = forward(tokens, upstream, norm_gain, w_up, bias_up, w_down, bias_down)
        out_d, out_u, out_s = backward(data_axis, g, gb, a, u, n, h, w_down, w_up, norm_gain)[:3]
        num_layers, width = norm_gain.shape
        blocks = bias_up.shape[1] // width
        per = blocks + 2
        layers = out_s[: num_layers * per].reshape(num_layers, per, width)
        return (layers[:, 0], out_u, layers[:, 1 : 1 + blocks].reshape(num_layers, blocks * width), out_d, layers[:, 1 + blocks])

    row_spec = P(data_axis, None)
    full_spec = P()
    return jax.shard_map(
        device_grads,
        mesh=mesh,
        in_specs=(row_spec, row_spec, full_spec, full_spec, full_spec, full_spec, full_spec),
        out_specs=(full_spec, full_spec, full_spec, full_spec, full_spec),
        check_vma=False,
    )
```

```python
import functools

import jax
import jax.numpy as jnp
from jax import lax
from jax.experimental import pallas as pl
from jax.experimental.pallas import tpu as pltpu
from jax.sharding import PartitionSpec as P

EPSILON = 1e-6
GELU_C = 0.7978845608028654
GELU_A = 0.044715
MESH = pl.DeviceIdType.MESH
bf16 = jnp.bfloat16
f32 = jnp.float32

ROW_TILE = 512
CHUNK = 512
SET_ROWS = 64
LAG = 2
SLOTS = 10
FIN_SLOTS = 16
STAGES = 11


def gelu_f32(u):
    inner = u * (GELU_C + (GELU_C * GELU_A) * (u * u))
    half = 0.5 * u
    return half + half * jnp.tanh(inner)


def row_of(ref, layer):
    both = ref[...].astype(f32)
    return jnp.where(layer == 0, both[0:1, :], both[1:2, :])


def forward_kernel(tok, up, gain, wu, bu, wd, bd, u_out, a_out, h_out, n_out, g_out, gb_out, hid):
    layer = pl.program_id(0)
    r = pl.program_id(1)
    rows = pl.ds(pl.multiple_of(r * ROW_TILE, ROW_TILE), ROW_TILE)

    @pl.when(layer == 0)
    def _():
        hid[rows, :] = tok[...]

    xb = hid[rows, :]
    x = xb.astype(f32)
    scale = lax.rsqrt(jnp.mean(x * x, axis=-1, keepdims=True) + EPSILON)
    n = ((x * scale) * row_of(gain, layer)).astype(bf16)
    bu_row = row_of(bu, layer)
    h_out[0] = xb
    n_out[0] = n
    hidden = wu.shape[2]
    acc = None
    for j in range(hidden // CHUNK):
        cols = pl.ds(j * CHUNK, CHUNK)
        pre = jnp.dot(n, wu[0, :, cols], preferred_element_type=f32) + bu_row[:, j * CHUNK : (j + 1) * CHUNK]
        u = pre.astype(bf16)
        u_out[0, :, cols] = u
        a = gelu_f32(u.astype(f32)).astype(bf16)
        a_out[0, :, cols] = a
        part = jnp.dot(a, wd[0, cols, :], preferred_element_type=f32)
        acc = part if acc is None else acc + part
    new = ((x + acc) + row_of(bd, layer)).astype(bf16)
    hid[rows, :] = new

    @pl.when(layer == 1)
    def _():
        top = new.astype(f32)
        s = lax.rsqrt(jnp.mean(top * top, axis=-1, keepdims=True) + EPSILON)
        zt = top * s
        upf = up[...].astype(f32)
        g = s * (upf - zt * jnp.mean(upf * zt, axis=-1, keepdims=True))
        g_out[...] = g
        gb_out[...] = g.astype(bf16)


def forward(tokens, upstream, norm_gain, w_up, bias_up, w_down, bias_down):
    rows, width = tokens.shape
    layers, _, hidden = w_up.shape
    tm = ROW_TILE
    grid = (layers, rows // tm)
    return pl.pallas_call(
        forward_kernel,
        name="forward",
        grid=grid,
        in_specs=[
            pl.BlockSpec((tm, width), lambda l, r: (r * (1 - l), 0)),
            pl.BlockSpec((tm, width), lambda l, r: (r * l, 0)),
            pl.BlockSpec((layers, width), lambda l, r: (0, 0)),
            pl.BlockSpec((1, width, hidden), lambda l, r: (l, 0, 0)),
            pl.BlockSpec((layers, hidden), lambda l, r: (0, 0)),
            pl.BlockSpec((1, hidden, width), lambda l, r: (l, 0, 0)),
            pl.BlockSpec((layers, width), lambda l, r: (0, 0)),
        ],
        out_specs=[
            pl.BlockSpec((1, tm, hidden), lambda l, r: (l, r, 0)),
            pl.BlockSpec((1, tm, hidden), lambda l, r: (l, r, 0)),
            pl.BlockSpec((1, tm, width), lambda l, r: (l, r, 0)),
            pl.BlockSpec((1, tm, width), lambda l, r: (l, r, 0)),
            pl.BlockSpec((tm, width), lambda l, r: (r * l, 0)),
            pl.BlockSpec((tm, width), lambda l, r: (r * l, 0)),
        ],
        out_shape=[
            jax.ShapeDtypeStruct((layers, rows, hidden), bf16),
            jax.ShapeDtypeStruct((layers, rows, hidden), bf16),
            jax.ShapeDtypeStruct((layers, rows, width), bf16),
            jax.ShapeDtypeStruct((layers, rows, width), bf16),
            jax.ShapeDtypeStruct((rows, width), f32),
            jax.ShapeDtypeStruct((rows, width), bf16),
        ],
        scratch_shapes=[pltpu.VMEM((rows, width), bf16)],
        compiler_params=pltpu.CompilerParams(vmem_limit_bytes=60 * 1024 * 1024, dimension_semantics=("arbitrary", "arbitrary")),
    )(tokens, upstream, norm_gain, w_up, bias_up, w_down, bias_down)


def backward_kernel(axis, num_sets, per_mat, g_hbm, gb_hbm, a_hbm, u_hbm, n_hbm, h_hbm, wd_hbm, wu_hbm, gain,
                    out_d, out_u, out_s, part_d, part_u, part_s,
                    acc, fin, land0, land1, land2, land3, land4, land5,
                    g, gb, m, xbuf, nbuf, hbuf, wd, wu, dbuf, rbuf, sbuf,
                    send_sem, recv_sem, loc_sem, x_sem, w_sem, r_sem, in_sem):
    width = acc.shape[2]
    half = SET_ROWS // 2
    piece = SET_ROWS // 8
    me = lax.axis_index(axis)
    core = lax.rem(me, 2)
    x = lax.rem(me // 2, 2)
    y = lax.rem(me // 4, 2)
    z = me // 8
    side = z // 2
    inner = jnp.logical_or(z == 1, z == 2)
    outer = jnp.logical_not(inner)
    b1 = jnp.where(core == 0, x, y)
    step1 = jnp.where(core == 0, 2, 4)
    b2 = jnp.where(core == 0, y, x)
    step2 = jnp.where(core == 0, 4, 2)
    partner = me + 1 - 2 * core
    near1 = me + step1 * (1 - 2 * b1)
    near2 = me + step2 * (1 - 2 * b2)
    zpair = me + 8 * (1 - 2 * lax.rem(z, 2))
    zmid = me + 8 * (3 - 2 * z)

    own_half = pl.multiple_of(b1 * half, 8)
    far_half = pl.multiple_of((1 - b1) * half, 8)
    start3 = pl.multiple_of(own_half + (1 - side) * piece, 8)
    far2 = pl.multiple_of(own_half + (1 - side) * 2 * piece, 8)
    near_2 = pl.multiple_of(own_half + side * 2 * piece, 8)
    outer_piece = pl.multiple_of(own_half + side * 3 * piece, 8)
    own_piece = pl.multiple_of(own_half + z * piece, 8)

    def slot_of(k):
        return lax.rem(k, SLOTS)

    def copy_to(stage, k, src, dst, peer):
        slot = slot_of(k)
        return pltpu.make_async_remote_copy(
            src_ref=src, dst_ref=dst, send_sem=send_sem.at[stage, slot], recv_sem=recv_sem.at[stage, slot],
            device_id=(peer,), device_id_type=MESH)

    def rows_of(k, base, n):
        return acc.at[lax.rem(k, FIN_SLOTS), pl.ds(base, n), :]

    def done_of(k, base, n):
        return fin.at[lax.rem(k, FIN_SLOTS), pl.ds(base, n), :]

    def add_rows(k, base, n, land):
        slot = lax.rem(k, FIN_SLOTS)
        acc[slot, pl.ds(base, n), :] = acc[slot, pl.ds(base, n), :] + land[slot_of(k)]

    def place(kind, j, who):
        if kind == 0:
            return pl.ds(pl.multiple_of(j * 2 * SET_ROWS + who * SET_ROWS, SET_ROWS), SET_ROWS), pl.ds(0, width)
        blocks = width // (2 * SET_ROWS)
        col = pl.multiple_of((j // blocks) * width, width)
        row = pl.multiple_of(lax.rem(j, blocks) * 2 * SET_ROWS + who * SET_ROWS, SET_ROWS)
        return pl.ds(row, SET_ROWS), pl.ds(col, width)

    def by_matrix(k, fn):
        mat = k // per_mat
        j = lax.rem(k, per_mat)
        for kind in range(2):
            @pl.when(jnp.logical_and(mat < 4, lax.rem(mat, 2) == kind))
            def _(kind=kind):
                fn(kind, (1 - mat // 2, j))

        @pl.when(mat >= 4)
        def _():
            fn(2, None)

    def part_of(refs, kind, where, who):
        if kind == 2:
            return refs[2].at[pl.ds(pl.multiple_of(who * SET_ROWS, SET_ROWS), SET_ROWS), :]
        rows, cols = place(kind, where[1], who)
        return refs[kind].at[where[0], rows, cols]

    def source(kind, where, who):
        return part_of((part_d, part_u, part_s), kind, where, who)

    def target(kind, where, who):
        return part_of((out_d, out_u, out_s), kind, where, who)

    def c_pair(k, kind=2, where=None):
        return copy_to(0, k, source(kind, where, 1 - core), land0.at[slot_of(k)], partner)

    def c_mine(k, kind=2, where=None):
        return pltpu.make_async_copy(source(kind, where, core), acc.at[lax.rem(k, FIN_SLOTS)], loc_sem.at[0, slot_of(k)])

    def c_d1(k):
        return copy_to(1, k, rows_of(k, far_half, half), land1.at[slot_of(k)], near1)

    def c_za(k):
        return copy_to(2, k, rows_of(k, start3, 3 * piece), land2.at[slot_of(k)], zpair)

    def c_zb(k):
        return copy_to(3, k, rows_of(k, far2, 2 * piece), land3.at[slot_of(k)], zmid)

    def c_zc(k):
        return copy_to(4, k, rows_of(k, outer_piece, piece), land4.at[slot_of(k)], zpair)

    def c_d2(k):
        return copy_to(5, k, rows_of(k, own_piece, piece), land5.at[slot_of(k)], near2)

    def c_zd(k):
        return copy_to(6, k, done_of(k, outer_piece, piece), done_of(k, outer_piece, piece), zpair)

    def c_ze(k):
        return copy_to(7, k, done_of(k, near_2, 2 * piece), done_of(k, near_2, 2 * piece), zmid)

    def c_zf(k):
        return copy_to(8, k, done_of(k, start3, 3 * piece), done_of(k, start3, 3 * piece), zpair)

    def c_e1(k):
        return copy_to(9, k, done_of(k, own_half, half), done_of(k, own_half, half), near1)

    def c_out(k, kind=2, where=None):
        return copy_to(10, k, done_of(k, 0, SET_ROWS), target(kind, where, core), partner)

    def c_loc(k, kind=2, where=None):
        return pltpu.make_async_copy(done_of(k, 0, SET_ROWS), target(kind, where, core), loc_sem.at[1, slot_of(k)])

    def wait0(k):
        pass

    def send0(k):
        def go(kind, where):
            c_pair(k, kind, where).start()
            c_mine(k, kind, where).start()
        by_matrix(k, go)

    def wait1(k):
        c_pair(k).wait()
        c_mine(k).wait()
        add_rows(k, 0, SET_ROWS, land0)

    def send1(k):
        c_d1(k).start()

    def wait2(k):
        c_d1(k).wait()
        add_rows(k, own_half, half, land1)

    def send2(k):
        @pl.when(outer)
        def _():
            c_za(k).start()

    def wait3(k):
        @pl.when(inner)
        def _():
            c_za(k).wait_recv()
            add_rows(k, start3, 3 * piece, land2)

        @pl.when(outer)
        def _():
            c_za(k).wait_send()

    def send3(k):
        @pl.when(inner)
        def _():
            c_zb(k).start()

    def wait4(k):
        @pl.when(inner)
        def _():
            c_zb(k).wait()
            add_rows(k, near_2, 2 * piece, land3)

    def send4(k):
        @pl.when(inner)
        def _():
            c_zc(k).start()

    def wait5(k):
        @pl.when(inner)
        def _():
            c_zc(k).wait_send()

        @pl.when(outer)
        def _():
            c_zc(k).wait_recv()
            add_rows(k, outer_piece, piece, land4)

    def send5(k):
        c_d2(k).start()

    def wait6(k):
        c_d2(k).wait()
        slot = lax.rem(k, FIN_SLOTS)
        fin[slot, pl.ds(own_piece, piece), :] = acc[slot, pl.ds(own_piece, piece), :] + land5[slot_of(k)]

    def send6(k):
        @pl.when(outer)
        def _():
            c_zd(k).start()

    def wait7(k):
        @pl.when(inner)
        def _():
            c_zd(k).wait_recv()

        @pl.when(outer)
        def _():
            c_zd(k).wait_send()

    def send7(k):
        @pl.when(inner)
        def _():
            c_ze(k).start()

    def wait8(k):
        @pl.when(inner)
        def _():
            c_ze(k).wait()

    def send8(k):
        @pl.when(inner)
        def _():
            c_zf(k).start()

    def wait9(k):
        @pl.when(inner)
        def _():
            c_zf(k).wait_send()

        @pl.when(outer)
        def _():
            c_zf(k).wait_recv()

    def send9(k):
        c_e1(k).start()

    def wait10(k):
        c_e1(k).wait()

    def send10(k):
        def go(kind, where):
            c_out(k, kind, where).start()
            c_loc(k, kind, where).start()
        by_matrix(k, go)

    def wait11(k):
        c_out(k).wait()
        c_loc(k).wait()

    def send11(k):
        pass

    waits = [wait0, wait1, wait2, wait3, wait4, wait5, wait6, wait7, wait8, wait9, wait10, wait11]
    sends = [send0, send1, send2, send3, send4, send5, send6, send7, send8, send9, send10, send11]

    def tick(t):
        for stage in range(STAGES + 1):
            k = t - stage * LAG

            @pl.when(jnp.logical_and(k >= 0, k < num_sets))
            def _(k=k, stage=stage):
                waits[stage](k)
                sends[stage](k)


    rows = g.shape[0]
    blocks = per_mat * 2 * SET_ROWS // width
    half_w = width // 2
    a_steps = 2 * blocks
    b_steps = 8 * blocks
    c_steps = 4
    layer_steps = a_steps + b_steps + c_steps
    all_steps = 2 * layer_steps
    tile = rows // 4
    small_rows = blocks + 2

    def load_x(q):
        layer = 1 - q // (2 * blocks)
        cols = pl.ds(pl.multiple_of(lax.rem(q, blocks) * width, width), width)
        for kind, ref in enumerate((a_hbm, u_hbm)):
            @pl.when(jnp.logical_and(q < 4 * blocks, lax.rem(q // blocks, 2) == kind))
            def _(ref=ref):
                pltpu.make_async_copy(ref.at[layer, :, cols], xbuf.at[lax.rem(q, 2)], x_sem.at[lax.rem(q, 2)]).start()

    def wait_x(q):
        pltpu.make_async_copy(a_hbm.at[0, :, pl.ds(0, width)], xbuf.at[lax.rem(q, 2)], x_sem.at[lax.rem(q, 2)]).wait()

    def w_copies(p):
        slot = lax.rem(p, 2)
        layer = 1 - p // blocks
        span = pl.ds(pl.multiple_of(lax.rem(p, blocks) * width, width), width)
        return (pltpu.make_async_copy(wd_hbm.at[layer, span, :], wd.at[slot], w_sem.at[0, slot]),
                pltpu.make_async_copy(wu_hbm.at[layer, :, span], wu.at[slot], w_sem.at[1, slot]))

    def layer_copies(layer):
        return (pltpu.make_async_copy(n_hbm.at[layer], nbuf, in_sem.at[2]), pltpu.make_async_copy(h_hbm.at[layer], hbuf, in_sem.at[3]))

    def result_wait(slot):
        pltpu.make_async_copy(rbuf.at[slot], part_d.at[0, pl.ds(0, half_w), :], r_sem.at[slot]).wait()

    load_gb = pltpu.make_async_copy(gb_hbm, gb, in_sem.at[0])
    load_g = pltpu.make_async_copy(g_hbm, g, in_sem.at[1])
    load_x(jnp.int32(0))
    load_gb.start()
    load_x(jnp.int32(1))
    for copy in w_copies(jnp.int32(0)):
        copy.start()
    load_g.start()
    barrier = pltpu.get_barrier_semaphore()
    for peer in (partner, near1, near2, zpair):
        pl.semaphore_signal(barrier, inc=1, device_id=(peer,), device_id_type=MESH)

    @pl.when(inner)
    def _():
        pl.semaphore_signal(barrier, inc=1, device_id=(zmid,), device_id_type=MESH)

    pl.semaphore_wait(barrier, jnp.where(inner, 5, 4))

    sbuf[...] = jnp.zeros_like(sbuf)
    load_gb.wait()

    def step_a(layer, w, r):
        slot = lax.rem(w, 2)
        block = w // 2
        q = (1 - layer) * 2 * blocks + block

        @pl.when(w == 0)
        def _():
            for copy in layer_copies(layer):
                copy.start()
            m[...] = jnp.zeros_like(m)

        @pl.when(slot == 0)
        def _():
            wait_x(q)

        @pl.when(r >= 2)
        def _():
            result_wait(slot)

        cols = pl.ds(pl.multiple_of(slot * half_w, 128), half_w)
        rbuf[slot] = lax.dot_general(xbuf[lax.rem(q, 2), :, cols], gb[...], (((0,), (0,)), ((), ())), preferred_element_type=f32)
        out_rows = pl.ds(pl.multiple_of(w * half_w, 128), half_w)
        pltpu.make_async_copy(rbuf.at[slot], part_d.at[layer, out_rows, :], r_sem.at[slot]).start()

        @pl.when(slot == 1)
        def _():
            load_x(q + 2)

    def step_e(layer, block, i):
        q = (1 - layer) * 2 * blocks + blocks + block
        p = (1 - layer) * blocks + block

        @pl.when(i == 0)
        def _():
            wait_x(q)
            for copy in w_copies(p):
                copy.wait()

            @pl.when(p + 1 < 2 * blocks)
            def _():
                for copy in w_copies(p + 1):
                    copy.start()

        span = pl.ds(pl.multiple_of(i * tile, 16), tile)
        e = lax.dot_general(gb[span, :], wd[lax.rem(p, 2)], (((1,), (1,)), ((), ())), preferred_element_type=f32)
        u = xbuf[lax.rem(q, 2), span, :].astype(f32)
        sq = u * u
        t = jnp.tanh(u * (GELU_C + (GELU_C * GELU_A) * sq))
        slope = ((1.0 - t * t) * (0.5 * u)) * (GELU_C + (3.0 * GELU_C * GELU_A) * sq) + (0.5 + 0.5 * t)
        d = e * slope
        dbuf[span, :] = d.astype(bf16)
        total = jnp.sum(d, axis=0, keepdims=True)
        row = pl.ds(layer * small_rows + 1 + block, 1)
        sbuf[row, :] = sbuf[row, :] + total

        @pl.when(i == 3)
        def _():
            load_x(q + 2)

    def step_m(layer, block, i):
        p = (1 - layer) * blocks + block
        span = pl.ds(pl.multiple_of(i * 2 * tile, 16), 2 * tile)
        m[span, :] = m[span, :] + lax.dot_general(dbuf[span, :], wu[lax.rem(p, 2)], (((1,), (1,)), ((), ())), preferred_element_type=f32)

    def step_u(layer, block, i):
        @pl.when(jnp.logical_and(block == 0, i == 0))
        def _():
            for copy in layer_copies(layer):
                copy.wait()

        result_wait(i)
        cols = pl.ds(pl.multiple_of(i * half_w, 128), half_w)
        rbuf[i] = lax.dot_general(nbuf[:, cols], dbuf[...], (((0,), (0,)), ((), ())), preferred_element_type=f32)
        out_cols = pl.ds(pl.multiple_of(block * width, width), width)
        pltpu.make_async_copy(rbuf.at[i], part_u.at[layer, cols, out_cols], r_sem.at[i]).start()

    def step_c(layer, i):
        @pl.when(jnp.logical_and(layer == 1, i == 0))
        def _():
            load_g.wait()

        span = pl.ds(pl.multiple_of(i * tile, 16), tile)
        x = hbuf[span, :].astype(f32)
        scale = lax.rsqrt(jnp.mean(x * x, axis=-1, keepdims=True) + EPSILON)
        hat = x * scale
        grad_n = m[span, :]
        old = g[span, :]
        gain_row = pl.ds(layer * small_rows, 1)
        bias_row = pl.ds(layer * small_rows + blocks + 1, 1)
        sbuf[gain_row, :] = sbuf[gain_row, :] + jnp.sum(grad_n * hat, axis=0, keepdims=True)
        sbuf[bias_row, :] = sbuf[bias_row, :] + jnp.sum(old, axis=0, keepdims=True)
        grad_hat = grad_n * row_of(gain, layer)
        new = old + scale * (grad_hat - hat * jnp.mean(grad_hat * hat, axis=-1, keepdims=True))
        g[span, :] = new
        gb[span, :] = new.astype(bf16)

    def compute(s):
        layer = 1 - s // layer_steps
        w = lax.rem(s, layer_steps)
        v = w - a_steps
        block = v // 8
        in_block = lax.rem(v, 8)
        r = (1 - layer) * 4 * blocks + w

        @pl.when(w < a_steps)
        def _():
            step_a(layer, w, r)

        in_b = jnp.logical_and(v >= 0, v < b_steps)
        for step, first, last in ((step_e, 0, 4), (step_m, 4, 6), (step_u, 6, 8)):
            @pl.when(jnp.logical_and(in_b, jnp.logical_and(in_block >= first, in_block < last)))
            def _(step=step, first=first):
                step(layer, block, in_block - first)

        @pl.when(v >= b_steps)
        def _():
            step_c(layer, v - b_steps)

    small_copy = pltpu.make_async_copy(sbuf, part_s, in_sem.at[4])

    def whole_step(s):
        @pl.when(s < all_steps)
        def _():
            compute(s)

        @pl.when(s == all_steps)
        def _():
            small_copy.start()
            result_wait(0)
            result_wait(1)
            small_copy.wait()

        @pl.when(s >= 2)
        def _():
            tick(s - 2)

    pl.loop(0, num_sets + STAGES * LAG + 2)(whole_step)


def backward(axis, g, gb, a, u, n, h, w_down, w_up, norm_gain):
    rows, width = g.shape
    hidden = a.shape[2]
    per_mat = hidden // (2 * SET_ROWS)
    num_sets = 4 * per_mat + 1
    piece = SET_ROWS // 8
    any_spec = pl.BlockSpec(memory_space=pl.ANY)
    shape = jax.ShapeDtypeStruct
    shapes = [shape((2, hidden, width), f32), shape((2, width, hidden), f32), shape((2 * SET_ROWS, width), f32)]
    return pl.pallas_call(
        functools.partial(backward_kernel, axis, num_sets, per_mat),
        name="backward_and_sum",
        out_shape=shapes + shapes,
        in_specs=[any_spec] * 8 + [pl.BlockSpec(memory_space=pltpu.VMEM)],
        out_specs=[any_spec] * 6,
        scratch_shapes=[
            pltpu.VMEM((FIN_SLOTS, SET_ROWS, width), f32),
            pltpu.VMEM((FIN_SLOTS, SET_ROWS, width), f32),
            pltpu.VMEM((SLOTS, SET_ROWS, width), f32),
            pltpu.VMEM((SLOTS, SET_ROWS // 2, width), f32),
            pltpu.VMEM((SLOTS, 3 * piece, width), f32),
            pltpu.VMEM((SLOTS, 2 * piece, width), f32),
            pltpu.VMEM((SLOTS, piece, width), f32),
            pltpu.VMEM((SLOTS, piece, width), f32),
            pltpu.VMEM((rows, width), f32),
            pltpu.VMEM((rows, width), bf16),
            pltpu.VMEM((rows, width), f32),
            pltpu.VMEM((2, rows, width), bf16),
            pltpu.VMEM((rows, width), bf16),
            pltpu.VMEM((rows, width), bf16),
            pltpu.VMEM((2, width, width), bf16),
            pltpu.VMEM((2, width, width), bf16),
            pltpu.VMEM((rows, width), bf16),
            pltpu.VMEM((2, width // 2, width), f32),
            pltpu.VMEM((2 * SET_ROWS, width), f32),
            pltpu.SemaphoreType.DMA((STAGES, SLOTS)),
            pltpu.SemaphoreType.DMA((STAGES, SLOTS)),
            pltpu.SemaphoreType.DMA((2, SLOTS)),
            pltpu.SemaphoreType.DMA((2,)),
            pltpu.SemaphoreType.DMA((2, 2)),
            pltpu.SemaphoreType.DMA((2,)),
            pltpu.SemaphoreType.DMA((5,)),
        ],
        compiler_params=pltpu.CompilerParams(collective_id=0, has_side_effects=True, vmem_limit_bytes=62 * 1024 * 1024),
    )(g, gb, a, u, n, h, w_down, w_up, norm_gain)


OUT_RING = 8


def emit_kernel(sum_d, sum_u, sum_s, gain_out, up_out, bias_up_out, down_out, bias_down_out, ring_d, ring_u, rows, sem_in, sem_out, sem_s):
    layers, hidden, width = sum_d.shape
    blocks = hidden // width
    per = blocks + 2
    small = pltpu.make_async_copy(sum_s.at[pl.ds(0, rows.shape[0]), :], rows, sem_s)
    small.start()
    down_rows = ring_d.shape[1]
    up_rows = ring_u.shape[1]
    jobs = []
    for layer in range(layers):
        for part in range(hidden // down_rows):
            span = pl.ds(part * down_rows, down_rows)
            jobs.append((sum_d.at[layer, span, :], ring_d, down_out.at[layer, span, :], 0))
            span = pl.ds(part * up_rows, up_rows)
            jobs.append((sum_u.at[layer, span, :], ring_u, up_out.at[layer, span, :], 1))
    reads, writes = [], []
    for number, (src, ring, dst, which) in enumerate(jobs):
        slot = (number // 2) % OUT_RING
        reads.append(pltpu.make_async_copy(src, ring.at[slot], sem_in.at[which, slot]))
        writes.append(pltpu.make_async_copy(ring.at[slot], dst, sem_out.at[which, slot]))
    ahead = 2 * OUT_RING
    lead = ahead - 4
    for number in range(min(lead, len(jobs))):
        reads[number].start()
    for number in range(len(jobs)):
        reads[number].wait()
        writes[number].start()
        follow = number + lead
        if follow < len(jobs):
            if follow >= ahead:
                writes[follow - ahead].wait()
            reads[follow].start()
        if number == 2:
            small.wait()
            for layer in range(layers):
                base = layer * per
                gain_out[layer : layer + 1, :] = rows[base : base + 1, :]
                bias_down_out[layer : layer + 1, :] = rows[base + blocks + 1 : base + blocks + 2, :]
                for block in range(blocks):
                    bias_up_out[layer : layer + 1, block * width : (block + 1) * width] = rows[base + 1 + block : base + 2 + block, :]
    for number in range(max(0, len(jobs) - ahead), len(jobs)):
        writes[number].wait()


def emit(sum_d, sum_u, sum_s):
    layers, hidden, width = sum_d.shape
    blocks = hidden // width
    any_spec = pl.BlockSpec(memory_space=pl.ANY)
    vmem_spec = pl.BlockSpec(memory_space=pltpu.VMEM)
    shape = jax.ShapeDtypeStruct
    return pl.pallas_call(
        emit_kernel,
        name="emit",
        out_shape=[shape((layers, width), f32), shape((layers, width, hidden), f32), shape((layers, hidden), f32),
                   shape((layers, hidden, width), f32), shape((layers, width), f32)],
        in_specs=[any_spec] * 3,
        out_specs=[vmem_spec, any_spec, vmem_spec, any_spec, vmem_spec],
        scratch_shapes=[
            pltpu.VMEM((OUT_RING, hidden // 8, width), f32),
            pltpu.VMEM((OUT_RING, width // 8, hidden), f32),
            pltpu.VMEM((8 * ((layers * (blocks + 2) + 7) // 8), width), f32),
            pltpu.SemaphoreType.DMA((2, OUT_RING)),
            pltpu.SemaphoreType.DMA((2, OUT_RING)),
            pltpu.SemaphoreType.DMA,
        ],
        compiler_params=pltpu.CompilerParams(vmem_limit_bytes=60 * 1024 * 1024),
    )(sum_d, sum_u, sum_s)


def solution(mesh):
    data_axis = mesh.axis_names[0]

    def device_grads(tokens, upstream, norm_gain, w_up, bias_up, w_down, bias_down):
        u, a, h, n, g, gb = forward(tokens, upstream, norm_gain, w_up, bias_up, w_down, bias_down)
        out_d, out_u, out_s = backward(data_axis, g, gb, a, u, n, h, w_down, w_up, norm_gain)[:3]
        return tuple(emit(out_d, out_u, out_s))

    row_spec = P(data_axis, None)
    full_spec = P()
    return jax.shard_map(
        device_grads,
        mesh=mesh,
        in_specs=(row_spec, row_spec, full_spec, full_spec, full_spec, full_spec, full_spec),
        out_specs=(full_spec, full_spec, full_spec, full_spec, full_spec),
        check_vma=False,
    )
```

```python
import functools

import jax
import jax.numpy as jnp
from jax import lax
from jax.experimental import pallas as pl
from jax.experimental.pallas import tpu as pltpu
from jax.sharding import PartitionSpec as P

EPSILON = 1e-6
GELU_C = 0.7978845608028654
GELU_A = 0.044715
MESH = pl.DeviceIdType.MESH
bf16 = jnp.bfloat16
f32 = jnp.float32

ROW_TILE = 512
CHUNK = 512
SET_ROWS = 64
LAG = 2
SLOTS = 8
FIN_SLOTS = 14
STAGES = 11


def gelu_f32(u):
    inner = u * (GELU_C + (GELU_C * GELU_A) * (u * u))
    half = 0.5 * u
    return half + half * jnp.tanh(inner)


def row_of(ref, layer):
    both = ref[...].astype(f32)
    return jnp.where(layer == 0, both[0:1, :], both[1:2, :])


def forward_kernel(tok, up, gain, wu, bu, wd, bd, u_out, a_out, h_out, n_out, g_out, gb_out, hid):
    layer = pl.program_id(0)
    r = pl.program_id(1)
    rows = pl.ds(pl.multiple_of(r * ROW_TILE, ROW_TILE), ROW_TILE)

    @pl.when(layer == 0)
    def _():
        hid[rows, :] = tok[...]

    xb = hid[rows, :]
    x = xb.astype(f32)
    scale = lax.rsqrt(jnp.mean(x * x, axis=-1, keepdims=True) + EPSILON)
    n = ((x * scale) * row_of(gain, layer)).astype(bf16)
    bu_row = row_of(bu, layer)
    h_out[0] = xb
    n_out[0] = n
    hidden = wu.shape[2]
    acc = None
    for j in range(hidden // CHUNK):
        cols = pl.ds(j * CHUNK, CHUNK)
        pre = jnp.dot(n, wu[0, :, cols], preferred_element_type=f32) + bu_row[:, j * CHUNK : (j + 1) * CHUNK]
        u = pre.astype(bf16)
        u_out[0, :, cols] = u
        a = gelu_f32(u.astype(f32)).astype(bf16)
        a_out[0, :, cols] = a
        part = jnp.dot(a, wd[0, cols, :], preferred_element_type=f32)
        acc = part if acc is None else acc + part
    new = ((x + acc) + row_of(bd, layer)).astype(bf16)
    hid[rows, :] = new

    @pl.when(layer == 1)
    def _():
        top = new.astype(f32)
        s = lax.rsqrt(jnp.mean(top * top, axis=-1, keepdims=True) + EPSILON)
        zt = top * s
        upf = up[...].astype(f32)
        g = s * (upf - zt * jnp.mean(upf * zt, axis=-1, keepdims=True))
        g_out[...] = g
        gb_out[...] = g.astype(bf16)


def forward(tokens, upstream, norm_gain, w_up, bias_up, w_down, bias_down):
    rows, width = tokens.shape
    layers, _, hidden = w_up.shape
    tm = ROW_TILE
    grid = (layers, rows // tm)
    return pl.pallas_call(
        forward_kernel,
        name="forward",
        grid=grid,
        in_specs=[
            pl.BlockSpec((tm, width), lambda l, r: (r * (1 - l), 0)),
            pl.BlockSpec((tm, width), lambda l, r: (r * l, 0)),
            pl.BlockSpec((layers, width), lambda l, r: (0, 0)),
            pl.BlockSpec((1, width, hidden), lambda l, r: (l, 0, 0)),
            pl.BlockSpec((layers, hidden), lambda l, r: (0, 0)),
            pl.BlockSpec((1, hidden, width), lambda l, r: (l, 0, 0)),
            pl.BlockSpec((layers, width), lambda l, r: (0, 0)),
        ],
        out_specs=[
            pl.BlockSpec((1, tm, hidden), lambda l, r: (l, r, 0)),
            pl.BlockSpec((1, tm, hidden), lambda l, r: (l, r, 0)),
            pl.BlockSpec((1, tm, width), lambda l, r: (l, r, 0)),
            pl.BlockSpec((1, tm, width), lambda l, r: (l, r, 0)),
            pl.BlockSpec((tm, width), lambda l, r: (r * l, 0)),
            pl.BlockSpec((tm, width), lambda l, r: (r * l, 0)),
        ],
        out_shape=[
            jax.ShapeDtypeStruct((layers, rows, hidden), bf16),
            jax.ShapeDtypeStruct((layers, rows, hidden), bf16),
            jax.ShapeDtypeStruct((layers, rows, width), bf16),
            jax.ShapeDtypeStruct((layers, rows, width), bf16),
            jax.ShapeDtypeStruct((rows, width), f32),
            jax.ShapeDtypeStruct((rows, width), bf16),
        ],
        scratch_shapes=[pltpu.VMEM((rows, width), bf16)],
        compiler_params=pltpu.CompilerParams(vmem_limit_bytes=60 * 1024 * 1024, dimension_semantics=("arbitrary", "arbitrary")),
    )(tokens, upstream, norm_gain, w_up, bias_up, w_down, bias_down)


def backward_kernel(axis, num_sets, per_mat, g_hbm, gb_hbm, a_hbm, u_hbm, n_hbm, h_hbm, wd_hbm, wu_hbm, gain,
                    out_d1, out_u1, out_v, out_s, part_d, part_u, part_s,
                    acc, fin, land0, land1, land2, land3, land4, land5,
                    gb, m, xbuf, nbuf, gtile, htile, wd, wu, dbuf, rbuf, sbuf,
                    send_sem, recv_sem, loc_sem, x_sem, w_sem, r_sem, in_sem):
    width = acc.shape[2]
    half = SET_ROWS // 2
    piece = SET_ROWS // 8
    me = lax.axis_index(axis)
    core = lax.rem(me, 2)
    x = lax.rem(me // 2, 2)
    y = lax.rem(me // 4, 2)
    z = me // 8
    side = z // 2
    inner = jnp.logical_or(z == 1, z == 2)
    outer = jnp.logical_not(inner)
    b1 = jnp.where(core == 0, x, y)
    step1 = jnp.where(core == 0, 2, 4)
    b2 = jnp.where(core == 0, y, x)
    step2 = jnp.where(core == 0, 4, 2)
    partner = me + 1 - 2 * core
    near1 = me + step1 * (1 - 2 * b1)
    near2 = me + step2 * (1 - 2 * b2)
    zpair = me + 8 * (1 - 2 * lax.rem(z, 2))
    zmid = me + 8 * (3 - 2 * z)

    own_half = pl.multiple_of(b1 * half, 8)
    far_half = pl.multiple_of((1 - b1) * half, 8)
    start3 = pl.multiple_of(own_half + (1 - side) * piece, 8)
    far2 = pl.multiple_of(own_half + (1 - side) * 2 * piece, 8)
    near_2 = pl.multiple_of(own_half + side * 2 * piece, 8)
    outer_piece = pl.multiple_of(own_half + side * 3 * piece, 8)
    own_piece = pl.multiple_of(own_half + z * piece, 8)

    def slot_of(k):
        return lax.rem(k, SLOTS)

    def copy_to(stage, k, src, dst, peer):
        slot = slot_of(k)
        return pltpu.make_async_remote_copy(
            src_ref=src, dst_ref=dst, send_sem=send_sem.at[stage, slot], recv_sem=recv_sem.at[stage, slot],
            device_id=(peer,), device_id_type=MESH)

    def rows_of(k, base, n):
        return acc.at[lax.rem(k, FIN_SLOTS), pl.ds(base, n), :]

    def done_of(k, base, n):
        return fin.at[lax.rem(k, FIN_SLOTS), pl.ds(base, n), :]

    def add_rows(k, base, n, land):
        slot = lax.rem(k, FIN_SLOTS)
        acc[slot, pl.ds(base, n), :] = acc[slot, pl.ds(base, n), :] + land[slot_of(k)]

    def place(kind, j, who):
        if kind == 0:
            return pl.ds(pl.multiple_of(j * 2 * SET_ROWS + who * SET_ROWS, SET_ROWS), SET_ROWS), pl.ds(0, width)
        blocks = width // (2 * SET_ROWS)
        col = pl.multiple_of((j // blocks) * width, width)
        row = pl.multiple_of(lax.rem(j, blocks) * 2 * SET_ROWS + who * SET_ROWS, SET_ROWS)
        return pl.ds(row, SET_ROWS), pl.ds(col, width)

    def by_matrix(k, fn):
        mat = k // per_mat
        j = lax.rem(k, per_mat)
        for number in range(5):
            @pl.when(mat == number)
            def _(number=number):
                fn(number, j)

    def part_of(refs, number, j, who):
        ref = refs[number]
        if number == 4:
            return ref.at[pl.ds(pl.multiple_of(who * SET_ROWS, SET_ROWS), SET_ROWS), :]
        rows, cols = place(number % 2, j, who)
        return ref.at[rows, cols]

    sources = (part_d.at[1], part_u.at[1], part_d.at[0], part_u.at[0], part_s)
    targets = (out_d1, out_u1, None, None, out_s)

    def rows_in_vmem(number, j, who):
        return pl.ds(pl.multiple_of(((number - 2) * per_mat + j) * 2 * SET_ROWS + who * SET_ROWS, SET_ROWS), SET_ROWS)

    def target(number, j, who):
        if number in (2, 3):
            return out_v.at[rows_in_vmem(number, j, who), :]
        return part_of(targets, number, j, who)

    def c_pair(k, number=4, j=0):
        return copy_to(0, k, part_of(sources, number, j, 1 - core), land0.at[slot_of(k)], partner)

    def c_mine(k, number=4, j=0):
        return pltpu.make_async_copy(part_of(sources, number, j, core), acc.at[lax.rem(k, FIN_SLOTS)], loc_sem.at[0, slot_of(k)])

    def c_d1(k):
        return copy_to(1, k, rows_of(k, far_half, half), land1.at[slot_of(k)], near1)

    def c_za(k):
        return copy_to(2, k, rows_of(k, start3, 3 * piece), land2.at[slot_of(k)], zpair)

    def c_zb(k):
        return copy_to(3, k, rows_of(k, far2, 2 * piece), land3.at[slot_of(k)], zmid)

    def c_zc(k):
        return copy_to(4, k, rows_of(k, outer_piece, piece), land4.at[slot_of(k)], zpair)

    def c_d2(k):
        return copy_to(5, k, rows_of(k, own_piece, piece), land5.at[slot_of(k)], near2)

    def c_zd(k):
        return copy_to(6, k, done_of(k, outer_piece, piece), done_of(k, outer_piece, piece), zpair)

    def c_ze(k):
        return copy_to(7, k, done_of(k, near_2, 2 * piece), done_of(k, near_2, 2 * piece), zmid)

    def c_zf(k):
        return copy_to(8, k, done_of(k, start3, 3 * piece), done_of(k, start3, 3 * piece), zpair)

    def c_e1(k):
        return copy_to(9, k, done_of(k, own_half, half), done_of(k, own_half, half), near1)

    def c_out(k, number=4, j=0):
        return copy_to(10, k, done_of(k, 0, SET_ROWS), target(number, j, core), partner)

    def c_loc(k, number=4, j=0):
        return pltpu.make_async_copy(done_of(k, 0, SET_ROWS), target(number, j, core), loc_sem.at[1, slot_of(k)])

    def wait0(k):
        pass

    def send0(k):
        def go(number, j):
            c_pair(k, number, j).start()
            c_mine(k, number, j).start()
        by_matrix(k, go)

    def wait1(k):
        c_pair(k).wait()
        c_mine(k).wait()
        add_rows(k, 0, SET_ROWS, land0)

    def send1(k):
        c_d1(k).start()

    def wait2(k):
        c_d1(k).wait()
        add_rows(k, own_half, half, land1)

    def send2(k):
        @pl.when(outer)
        def _():
            c_za(k).start()

    def wait3(k):
        @pl.when(inner)
        def _():
            c_za(k).wait_recv()
            add_rows(k, start3, 3 * piece, land2)

        @pl.when(outer)
        def _():
            c_za(k).wait_send()

    def send3(k):
        @pl.when(inner)
        def _():
            c_zb(k).start()

    def wait4(k):
        @pl.when(inner)
        def _():
            c_zb(k).wait()
            add_rows(k, near_2, 2 * piece, land3)

    def send4(k):
        @pl.when(inner)
        def _():
            c_zc(k).start()

    def wait5(k):
        @pl.when(inner)
        def _():
            c_zc(k).wait_send()

        @pl.when(outer)
        def _():
            c_zc(k).wait_recv()
            add_rows(k, outer_piece, piece, land4)

    def send5(k):
        c_d2(k).start()

    def wait6(k):
        c_d2(k).wait()
        slot = lax.rem(k, FIN_SLOTS)
        fin[slot, pl.ds(own_piece, piece), :] = acc[slot, pl.ds(own_piece, piece), :] + land5[slot_of(k)]

    def send6(k):
        @pl.when(outer)
        def _():
            c_zd(k).start()

    def wait7(k):
        @pl.when(inner)
        def _():
            c_zd(k).wait_recv()

        @pl.when(outer)
        def _():
            c_zd(k).wait_send()

    def send7(k):
        @pl.when(inner)
        def _():
            c_ze(k).start()

    def wait8(k):
        @pl.when(inner)
        def _():
            c_ze(k).wait()

    def send8(k):
        @pl.when(inner)
        def _():
            c_zf(k).start()

    def wait9(k):
        @pl.when(inner)
        def _():
            c_zf(k).wait_send()

        @pl.when(outer)
        def _():
            c_zf(k).wait_recv()

    def send9(k):
        c_e1(k).start()

    def wait10(k):
        c_e1(k).wait()

    def send10(k):
        def go(number, j):
            c_out(k, number, j).start()
            if number in (2, 3):
                out_v[rows_in_vmem(number, j, core), :] = fin[lax.rem(k, FIN_SLOTS)]
            else:
                c_loc(k, number, j).start()
        by_matrix(k, go)

    def wait11(k):
        c_out(k).wait()
        mat = k // per_mat

        @pl.when(jnp.logical_not(jnp.logical_or(mat == 2, mat == 3)))
        def _():
            c_loc(k).wait()

    def send11(k):
        pass

    waits = [wait0, wait1, wait2, wait3, wait4, wait5, wait6, wait7, wait8, wait9, wait10, wait11]
    sends = [send0, send1, send2, send3, send4, send5, send6, send7, send8, send9, send10, send11]

    def tick(t):
        for stage in range(STAGES + 1):
            k = t - stage * LAG

            @pl.when(jnp.logical_and(k >= 0, k < num_sets))
            def _(k=k, stage=stage):
                waits[stage](k)
                sends[stage](k)


    rows = gb.shape[0]
    blocks = per_mat * 2 * SET_ROWS // width
    half_w = width // 2
    a_steps = 2 * blocks
    b_steps = 8 * blocks
    c_steps = 4
    layer_steps = a_steps + b_steps + c_steps
    all_steps = 2 * layer_steps
    tile = rows // 4
    small_rows = blocks + 2

    def load_x(q):
        layer = 1 - q // (2 * blocks)
        cols = pl.ds(pl.multiple_of(lax.rem(q, blocks) * width, width), width)
        for kind, ref in enumerate((a_hbm, u_hbm)):
            @pl.when(jnp.logical_and(q < 4 * blocks, lax.rem(q // blocks, 2) == kind))
            def _(ref=ref):
                pltpu.make_async_copy(ref.at[layer, :, cols], xbuf.at[lax.rem(q, 2)], x_sem.at[lax.rem(q, 2)]).start()

    def wait_x(q):
        pltpu.make_async_copy(a_hbm.at[0, :, pl.ds(0, width)], xbuf.at[lax.rem(q, 2)], x_sem.at[lax.rem(q, 2)]).wait()

    def w_copy(which, p):
        layer = 1 - p // blocks
        span = pl.ds(pl.multiple_of(lax.rem(p, blocks) * width, width), width)
        if which == 0:
            return pltpu.make_async_copy(wd_hbm.at[layer, span, :], wd, w_sem.at[0])
        return pltpu.make_async_copy(wu_hbm.at[layer, :, span], wu, w_sem.at[1])

    def n_copy(layer):
        return pltpu.make_async_copy(n_hbm.at[layer], nbuf, in_sem.at[2])

    def h_copy(layer, i):
        span = pl.ds(pl.multiple_of(i * tile, 16), tile)
        return pltpu.make_async_copy(h_hbm.at[layer, span, :], htile, in_sem.at[3])

    def g_copy(i):
        span = pl.ds(pl.multiple_of(i * tile, 16), tile)
        return pltpu.make_async_copy(g_hbm.at[span, :], gtile, in_sem.at[1])

    def load_rows(layer, i):
        h_copy(layer, i).start()

        @pl.when(layer == 1)
        def _():
            g_copy(i).start()

    def result_wait(slot):
        pltpu.make_async_copy(rbuf.at[slot], part_d.at[0, pl.ds(0, half_w), :], r_sem.at[slot]).wait()

    load_gb = pltpu.make_async_copy(gb_hbm, gb, in_sem.at[0])
    load_x(jnp.int32(0))
    load_gb.start()
    load_x(jnp.int32(1))
    w_copy(0, jnp.int32(0)).start()
    w_copy(1, jnp.int32(0)).start()
    barrier = pltpu.get_barrier_semaphore()
    for peer in (partner, near1, near2, zpair):
        pl.semaphore_signal(barrier, inc=1, device_id=(peer,), device_id_type=MESH)

    @pl.when(inner)
    def _():
        pl.semaphore_signal(barrier, inc=1, device_id=(zmid,), device_id_type=MESH)

    pl.semaphore_wait(barrier, jnp.where(inner, 5, 4))

    sbuf[...] = jnp.zeros_like(sbuf)
    load_gb.wait()

    def step_a(layer, w, r):
        slot = lax.rem(w, 2)
        block = w // 2
        q = (1 - layer) * 2 * blocks + block

        @pl.when(w == 0)
        def _():
            n_copy(layer).start()
            m[...] = jnp.zeros_like(m)

        @pl.when(slot == 0)
        def _():
            wait_x(q)

        cols = pl.ds(pl.multiple_of(slot * half_w, 128), half_w)
        rbuf[slot] = lax.dot_general(xbuf[lax.rem(q, 2), :, cols], gb[...], (((0,), (0,)), ((), ())), preferred_element_type=f32)

        @pl.when(r >= 1)
        def _():
            result_wait(1 - slot)

        out_rows = pl.ds(pl.multiple_of(w * half_w, 128), half_w)
        pltpu.make_async_copy(rbuf.at[slot], part_d.at[layer, out_rows, :], r_sem.at[slot]).start()

        @pl.when(slot == 1)
        def _():
            load_x(q + 2)

    def step_e(layer, block, i):
        q = (1 - layer) * 2 * blocks + blocks + block
        p = (1 - layer) * blocks + block

        @pl.when(i == 0)
        def _():
            wait_x(q)
            w_copy(0, p).wait()

        span = pl.ds(pl.multiple_of(i * tile, 16), tile)
        e = lax.dot_general(gb[span, :], wd[...], (((1,), (1,)), ((), ())), preferred_element_type=f32)
        u = xbuf[lax.rem(q, 2), span, :].astype(f32)
        sq = u * u
        t = jnp.tanh(u * (GELU_C + (GELU_C * GELU_A) * sq))
        slope = ((1.0 - t * t) * (0.5 * u)) * (GELU_C + (3.0 * GELU_C * GELU_A) * sq) + (0.5 + 0.5 * t)
        d = e * slope
        dbuf[span, :] = d.astype(bf16)
        total = jnp.sum(d, axis=0, keepdims=True)
        row = pl.ds(layer * small_rows + 1 + block, 1)
        sbuf[row, :] = sbuf[row, :] + total

        @pl.when(i == 3)
        def _():
            load_x(q + 2)

            @pl.when(p + 1 < 2 * blocks)
            def _():
                w_copy(0, p + 1).start()

    def step_m(layer, block, i):
        p = (1 - layer) * blocks + block
        @pl.when(i == 0)
        def _():
            w_copy(1, p).wait()

        span = pl.ds(pl.multiple_of(i * 2 * tile, 16), 2 * tile)
        m[span, :] = m[span, :] + lax.dot_general(dbuf[span, :], wu[...], (((1,), (1,)), ((), ())), preferred_element_type=f32)

        @pl.when(jnp.logical_and(i == 1, p + 1 < 2 * blocks))
        def _():
            w_copy(1, p + 1).start()

    def step_u(layer, block, i):
        @pl.when(jnp.logical_and(block == 0, i == 0))
        def _():
            n_copy(layer).wait()

        cols = pl.ds(pl.multiple_of(i * half_w, 128), half_w)
        rbuf[i] = lax.dot_general(nbuf[:, cols], dbuf[...], (((0,), (0,)), ((), ())), preferred_element_type=f32)
        result_wait(1 - i)
        out_cols = pl.ds(pl.multiple_of(block * width, width), width)
        pltpu.make_async_copy(rbuf.at[i], part_u.at[layer, cols, out_cols], r_sem.at[i]).start()

        @pl.when(jnp.logical_and(block == blocks - 1, i == 1))
        def _():
            load_rows(layer, 0)

    def step_c(layer, i):
        span = pl.ds(pl.multiple_of(i * tile, 16), tile)
        h_copy(layer, i).wait()
        x = htile[...].astype(f32)
        scale = lax.rsqrt(jnp.mean(x * x, axis=-1, keepdims=True) + EPSILON)
        hat = x * scale
        grad_n = m[span, :]
        gain_row = pl.ds(layer * small_rows, 1)
        sbuf[gain_row, :] = sbuf[gain_row, :] + jnp.sum(grad_n * hat, axis=0, keepdims=True)

        @pl.when(layer == 1)
        def _():
            g_copy(i).wait()
            old = gtile[...]
            bias_row = small_rows + blocks + 1
            sbuf[bias_row : bias_row + 1, :] = sbuf[bias_row : bias_row + 1, :] + jnp.sum(old, axis=0, keepdims=True)
            grad_hat = grad_n * row_of(gain, layer)
            new = old + scale * (grad_hat - hat * jnp.mean(grad_hat * hat, axis=-1, keepdims=True))
            bias_row = blocks + 1
            sbuf[bias_row : bias_row + 1, :] = sbuf[bias_row : bias_row + 1, :] + jnp.sum(new, axis=0, keepdims=True)
            gb[span, :] = new.astype(bf16)

        @pl.when(i < 3)
        def _():
            load_rows(layer, i + 1)

    def compute(s):
        layer = 1 - s // layer_steps
        w = lax.rem(s, layer_steps)
        v = w - a_steps
        block = v // 8
        in_block = lax.rem(v, 8)
        r = (1 - layer) * 4 * blocks + w

        @pl.when(w < a_steps)
        def _():
            step_a(layer, w, r)

        in_b = jnp.logical_and(v >= 0, v < b_steps)
        for step, first, last in ((step_e, 0, 4), (step_m, 4, 6), (step_u, 6, 8)):
            @pl.when(jnp.logical_and(in_b, jnp.logical_and(in_block >= first, in_block < last)))
            def _(step=step, first=first):
                step(layer, block, in_block - first)

        @pl.when(v >= b_steps)
        def _():
            step_c(layer, v - b_steps)

    small_copy = pltpu.make_async_copy(sbuf, part_s, in_sem.at[4])

    def whole_step(s):
        @pl.when(s < all_steps)
        def _():
            compute(s)

        @pl.when(s == all_steps)
        def _():
            small_copy.start()
            result_wait(1)
            small_copy.wait()

        @pl.when(s >= 1)
        def _():
            tick(s - 1)

    pl.loop(0, num_sets + STAGES * LAG + 1)(whole_step)


def backward(axis, g, gb, a, u, n, h, w_down, w_up, norm_gain):
    rows, width = g.shape
    hidden = a.shape[2]
    per_mat = hidden // (2 * SET_ROWS)
    num_sets = 4 * per_mat + 1
    piece = SET_ROWS // 8
    any_spec = pl.BlockSpec(memory_space=pl.ANY)
    shape = jax.ShapeDtypeStruct
    small_shape = shape((2 * SET_ROWS, width), f32)
    shapes = [shape((hidden, width), f32), shape((width, hidden), f32), pltpu.VMEM((2 * hidden, width), f32), small_shape,
              shape((2, hidden, width), f32), shape((2, width, hidden), f32), small_shape]
    vmem_spec = pl.BlockSpec(memory_space=pltpu.VMEM)
    return pl.pallas_call(
        functools.partial(backward_kernel, axis, num_sets, per_mat),
        name="backward_and_sum",
        out_shape=shapes,
        in_specs=[any_spec] * 8 + [vmem_spec],
        out_specs=[any_spec] * 2 + [vmem_spec] + [any_spec] * 4,
        scratch_shapes=[
            pltpu.VMEM((FIN_SLOTS, SET_ROWS, width), f32),
            pltpu.VMEM((FIN_SLOTS, SET_ROWS, width), f32),
            pltpu.VMEM((SLOTS, SET_ROWS, width), f32),
            pltpu.VMEM((SLOTS, SET_ROWS // 2, width), f32),
            pltpu.VMEM((SLOTS, 3 * piece, width), f32),
            pltpu.VMEM((SLOTS, 2 * piece, width), f32),
            pltpu.VMEM((SLOTS, piece, width), f32),
            pltpu.VMEM((SLOTS, piece, width), f32),
            pltpu.VMEM((rows, width), bf16),
            pltpu.VMEM((rows, width), f32),
            pltpu.VMEM((2, rows, width), bf16),
            pltpu.VMEM((rows, width), bf16),
            pltpu.VMEM((rows // 4, width), f32),
            pltpu.VMEM((rows // 4, width), bf16),
            pltpu.VMEM((width, width), bf16),
            pltpu.VMEM((width, width), bf16),
            pltpu.VMEM((rows, width), bf16),
            pltpu.VMEM((2, width // 2, width), f32),
            pltpu.VMEM((2 * SET_ROWS, width), f32),
            pltpu.SemaphoreType.DMA((STAGES, SLOTS)),
            pltpu.SemaphoreType.DMA((STAGES, SLOTS)),
            pltpu.SemaphoreType.DMA((2, SLOTS)),
            pltpu.SemaphoreType.DMA((2,)),
            pltpu.SemaphoreType.DMA((2,)),
            pltpu.SemaphoreType.DMA((2,)),
            pltpu.SemaphoreType.DMA((5,)),
        ],
        compiler_params=pltpu.CompilerParams(collective_id=0, has_side_effects=True, vmem_limit_bytes=45 * 1024 * 1024),
    )(g, gb, a, u, n, h, w_down, w_up, norm_gain)


OUT_RING = 6


def emit_kernel(sum_d1, sum_u1, sum_v, sum_s, gain_out, up_out, bias_up_out, down_out, bias_down_out, ring_d, ring_u, rows, sem_in, sem_out, sem_s, sem_v):
    hidden, width = sum_d1.shape
    layers = 2
    blocks = hidden // width
    per = blocks + 2
    down_rows, up_rows = ring_d.shape[1], ring_u.shape[1]
    parts = hidden // down_rows
    jobs = []
    for part in range(parts):
        for which, (src, ring, dst, step) in enumerate(((sum_d1, ring_d, down_out, down_rows), (sum_u1, ring_u, up_out, up_rows))):
            span = pl.ds(part * step, step)
            slot = part % OUT_RING
            jobs.append((pltpu.make_async_copy(src.at[span, :], ring.at[slot], sem_in.at[which, slot]),
                         pltpu.make_async_copy(ring.at[slot], dst.at[1, span, :], sem_out.at[which, slot])))
    small = pltpu.make_async_copy(sum_s.at[pl.ds(0, rows.shape[0]), :], rows, sem_s)
    direct = []
    for block in range(blocks):
        span = pl.ds(block * width, width)
        direct.append(pltpu.make_async_copy(sum_v.at[span, :], down_out.at[0, span, :], sem_v.at[0, block]))
        direct.append(pltpu.make_async_copy(sum_v.at[pl.ds(hidden + block * width, width), :], up_out.at[0, :, span], sem_v.at[1, block]))
    ahead = 2 * OUT_RING
    lead = ahead - 4
    small.start()
    for number in range(min(lead, len(jobs))):
        jobs[number][0].start()
    for copy in direct:
        copy.start()
    small.wait()
    for layer in range(layers):
        base = layer * per
        gain_out[layer : layer + 1, :] = rows[base : base + 1, :]
        bias_down_out[layer : layer + 1, :] = rows[base + blocks + 1 : base + blocks + 2, :]
        for block in range(blocks):
            bias_up_out[layer : layer + 1, block * width : (block + 1) * width] = rows[base + 1 + block : base + 2 + block, :]
    for number in range(len(jobs)):
        jobs[number][0].wait()
        jobs[number][1].start()
        follow = number + lead
        if follow < len(jobs):
            if follow >= ahead:
                jobs[follow - ahead][1].wait()
            jobs[follow][0].start()
    for number in range(max(0, len(jobs) - ahead), len(jobs)):
        jobs[number][1].wait()
    for copy in direct:
        copy.wait()


def emit(sum_d1, sum_u1, sum_v, sum_s):
    hidden, width = sum_d1.shape
    layers = 2
    blocks = hidden // width
    any_spec = pl.BlockSpec(memory_space=pl.ANY)
    vmem_spec = pl.BlockSpec(memory_space=pltpu.VMEM)
    hbm_spec = pl.BlockSpec(memory_space=pltpu.HBM)
    shape = jax.ShapeDtypeStruct
    return pl.pallas_call(
        emit_kernel,
        name="emit",
        out_shape=[shape((layers, width), f32), shape((layers, width, hidden), f32), shape((layers, hidden), f32),
                   shape((layers, hidden, width), f32), shape((layers, width), f32)],
        in_specs=[hbm_spec] * 2 + [vmem_spec] + [hbm_spec],
        out_specs=[vmem_spec, any_spec, vmem_spec, any_spec, vmem_spec],
        scratch_shapes=[
            pltpu.VMEM((OUT_RING, hidden // 8, width), f32),
            pltpu.VMEM((OUT_RING, width // 8, hidden), f32),
            pltpu.VMEM((8 * ((layers * (blocks + 2) + 7) // 8), width), f32),
            pltpu.SemaphoreType.DMA((2, OUT_RING)),
            pltpu.SemaphoreType.DMA((2, OUT_RING)),
            pltpu.SemaphoreType.DMA,
            pltpu.SemaphoreType.DMA((2, blocks)),
        ],
        compiler_params=pltpu.CompilerParams(vmem_limit_bytes=40 * 1024 * 1024),
    )(sum_d1, sum_u1, pltpu.with_memory_space_constraint(sum_v, pltpu.VMEM), sum_s)


def solution(mesh):
    data_axis = mesh.axis_names[0]

    def device_grads(tokens, upstream, norm_gain, w_up, bias_up, w_down, bias_down):
        u, a, h, n, g, gb = forward(tokens, upstream, norm_gain, w_up, bias_up, w_down, bias_down)
        sums = backward(data_axis, g, gb, a, u, n, h, w_down, w_up, norm_gain)[:4]
        return tuple(emit(*sums))

    row_spec = P(data_axis, None)
    full_spec = P()
    return jax.shard_map(
        device_grads,
        mesh=mesh,
        in_specs=(row_spec, row_spec, full_spec, full_spec, full_spec, full_spec, full_spec),
        out_specs=(full_spec, full_spec, full_spec, full_spec, full_spec),
        check_vma=False,
    )
```
